256 devices in a mesh: dp: 32 (over z, x_hi, core), owner: 8 (over x_lo, y).
Axes of the slice: x: 4 (x_hi: 2, x_lo: 2; x = x_hi * 2 + x_lo), y: 4, z: 8, core: 2. Of those that a mesh axis runs over, the one named last changes fastest.
Arguments:
- edge_in: bfloat16 [8, 65536, 512], P(None, ('dp', 'owner')), may hold values from -256 to 256
- edge_grad: bfloat16 [8, 65536, 512], P(None, ('dp', 'owner')), may hold values from -1.1953125 to 1.1953125
- row_mask: int32 [8, 65536], P(None, ('dp', 'owner')), may hold values 0 or 1
- layer_at: int32 [8], replicated, may hold values from 0 to 7, each once
Outputs:
- update: bfloat16 [8, 512, 512], P('owner')
The draws below stay inside these ranges and needn't reach their ends.
Inputs may be any that keep to these rules, and one draw needn't show every extreme that they name: `layer_at`: every layer number appears once.
All inputs are finite; a program needn't handle non-finite values. No bound on the sum of `row_mask` on one device may be relied on, other than what follows from the above.
Results may differ from the reference program's by a relative error of at most 0.0085.
Values may be sent and summed in bfloat16 or wider, within the bound.
A program may use at most 64 MiB of HBM per device.

```python
import math
import jax
import jax.numpy as jnp
from jax import lax

D = 512
LAYERS = 8
ROWS_DEV = 256
ROWS_ALL = 65536
ITERS = 4


def draw_edge_in(key, part):
    base = jax.random.fold_in(key, 11)
    key_a, key_b = jax.random.split(base, 2)
    normal_part = jnp.clip(jax.random.normal(key_a, (LAYERS, ROWS_ALL, D), jnp.float32), -6.0, 6.0)
    unit = jax.random.uniform(key_b, (LAYERS, ROWS_ALL, 1), jnp.float32)
    scale = jnp.exp(unit * jnp.log(10.0))
    values = scale * normal_part
    return jnp.clip(values, -256.0, 256.0).astype(jnp.bfloat16)


def plant(entries, stream_key, least, largest):
    extent = entries.shape
    index_at = [jax.random.randint(jax.random.fold_in(stream_key, axis), (), 0, extent[axis]) for axis in range(len(extent))]
    entries = entries.at[tuple(index_at)].set(least)
    longest = extent.index(max(extent))
    index_at[longest] = (index_at[longest] + 1) % extent[longest]
    return entries.at[tuple(index_at)].set(largest)


def steps_of(own_key, shape, cuts, least, largest):
    def one(dim, parts):
        steps = jax.random.uniform(jax.random.fold_in(jax.random.fold_in(own_key, 6), dim), (parts,), jnp.float32, least / len(cuts), largest / len(cuts))
        return jnp.repeat(jnp.exp(steps), shape[dim] // parts).reshape((-1,) + (1,) * (len(shape) - dim - 1))

    gain = one(*cuts[0])
    for cut in cuts[1:]:
        gain = gain * one(*cut)
    return gain


def normal_values(stream_key, shape, deviation, bound, cuts=(), held_as=jnp.bfloat16):
    values = deviation * jax.random.normal(stream_key, shape, jnp.float32)
    if cuts:
        values = values * steps_of(stream_key, shape, cuts, -0.22, 0.18)
    return jnp.clip(values, -bound, bound).astype(held_as)


def setup_inputs(seed: int = 0) -> dict:
    key_list = jax.random.split(jax.random.key(seed), 5)
    return {
        "edge_in": draw_edge_in(jax.random.fold_in(key_list[4], 71), 0),
        "edge_grad": normal_values(key_list[1], (LAYERS, ROWS_ALL, D), 0.2, 1.1953125, ((1, 256),)),
        "row_mask": plant((jax.random.randint(key_list[2], (LAYERS, ROWS_ALL), 0, 2) < 1).astype(jnp.int32), jax.random.fold_in(key_list[2], 1), 0, 1),
        "layer_at": jax.random.permutation(key_list[3], LAYERS).astype(jnp.int32),
    }


def newton(factor):
    eye = jnp.eye(D, dtype=jnp.float32)
    damped = factor + jnp.trace(factor) * (0.05 / D) * eye
    size_sq = jnp.sqrt(jnp.sum(damped * damped) + 1e-06)
    approx = eye / size_sq
    for step in range(ITERS):
        inner = jnp.matmul(damped, approx, precision=lax.Precision.HIGHEST)
        approx = 2.0 * approx - jnp.matmul(approx, inner, precision=lax.Precision.HIGHEST)
    return approx

def precondition(packed):
    factor_in, factor_out, grad = packed
    inv_in = newton(factor_in)
    inv_out = newton(factor_out)
    left = jnp.matmul(inv_in, grad, precision=lax.Precision.HIGHEST)
    return jnp.matmul(left, inv_out, precision=lax.Precision.HIGHEST)

def reference(edge_in, edge_grad, row_mask, layer_at):
    scale_factor = 1.0 / ROWS_ALL
    scale_grad = 1.0 / math.sqrt(ROWS_ALL)

    def add_block(index, carry):
        total_in, total_out, total_grad = carry
        start = index * ROWS_DEV
        inputs = lax.dynamic_slice_in_dim(edge_in, start, ROWS_DEV, 1).astype(jnp.float32)
        grads = lax.dynamic_slice_in_dim(edge_grad, start, ROWS_DEV, 1).astype(jnp.float32)
        weights = lax.dynamic_slice_in_dim(row_mask, start, ROWS_DEV, 1).astype(jnp.float32)[..., None]
        kept_in = inputs * weights
        kept_grad = grads * weights
        term_in = (jnp.einsum('lrd,lre->lde', kept_in, kept_in) * scale_factor).astype(jnp.bfloat16)
        term_out = (jnp.einsum('lrd,lre->lde', kept_grad, kept_grad) * scale_factor).astype(jnp.bfloat16)
        term_grad = (jnp.einsum('lrd,lre->lde', inputs, grads) * scale_grad).astype(jnp.bfloat16)
        term_in, term_out, term_grad = lax.optimization_barrier((term_in, term_out, term_grad))
        return (total_in + term_in.astype(jnp.float32), total_out + term_out.astype(jnp.float32), total_grad + term_grad.astype(jnp.float32))
    zeros = jnp.zeros((LAYERS, D, D), jnp.float32)
    factor_in, factor_out, grad = lax.fori_loop(0, ROWS_ALL // ROWS_DEV, add_block, (zeros, zeros, zeros))
    picked = (jnp.take(factor_in, layer_at, axis=0), jnp.take(factor_out, layer_at, axis=0), jnp.take(grad, layer_at, axis=0))
    update = lax.map(precondition, picked)
    return update.astype(jnp.bfloat16)
```

```python
import jax
import jax.numpy as jnp
from jax import lax
from jax.experimental import pallas as pl
from jax.experimental.pallas import tpu as pltpu
from jax.sharding import PartitionSpec as P

MESH = pl.DeviceIdType.MESH
F32 = jnp.float32
BF16 = jnp.bfloat16
L = 8
D = 512
R = 256
NZ = 8
T = 128
UPPER = [(i, j) for i in range(4) for j in range(i, 4)]
FP = 16 * len(UPPER)
GP = 16 * 8


def add(a, b):
    return (a.astype(F32) + b.astype(F32)).astype(BF16)


def split(x):
    hi = x.astype(BF16)
    return hi, (x - hi.astype(F32)).astype(BF16)


def dot(a, b):
    return lax.dot_general(a, b, (((1,), (0,)), ((), ())), preferred_element_type=F32)


def dot3(a, b):
    (ah, al), (bh, bl) = a, b
    return dot(ah, bh) + (dot(ah, bl) + dot(al, bh))


class Sems:
    def __init__(self, send, recv):
        self.send, self.recv, self.used, self.open = send, recv, 0, []

    def take(self, n=1):
        base = self.used
        self.used += n
        return base


def kernel(
    layer_at, mask_hbm, in_hbm, grad_hbm, out,
    mask, A, B, AT, WF, WG, RFh, RFz, FY, RFy1, RFy2, FX, RFx, FH, RFxh, FA,
    RGy1, RGy2, GX, RGx, GZ, RGh, RGz, GH, RGxh, GA, GAp,
    Fm, Pm, Qm, Xh, Xl, XPh, XPl, local_sem, send_sem, recv_sem,
):
    dp, ow = lax.axis_index("dp"), lax.axis_index("owner")
    z, xh, c = dp // 4, (dp // 2) % 2, dp % 2
    xl, y = ow // 4, ow % 4

    def dev(z=z, xh=xh, c=c, xl=xl, y=y):
        return (z * 4 + xh * 2 + c, xl * 4 + y)

    ya = y + 1 - 2 * (y % 2)
    yb = 3 - y
    core = dev(c=1 - c)
    dev_ya, dev_yb = dev(y=ya), dev(y=yb)
    dev_x, dev_xh = dev(xl=1 - xl), dev(xh=1 - xh)
    up, down = dev(z=(z + 1) % NZ), dev(z=(z + NZ - 1) % NZ)

    used = [0]

    def ids(n=1):
        used[0] += n
        return used[0] - n

    pending = []

    def remote(src, dst, k, to):
        return pltpu.make_async_remote_copy(
            src_ref=src, dst_ref=dst, send_sem=send_sem.at[k], recv_sem=recv_sem.at[k],
            device_id=to, device_id_type=MESH,
        )

    def send(src, dst, k, to):
        remote(src, dst, k, to).start()
        pending.append((src, dst, k, to))

    def arrived(dst, k):
        remote(dst, dst, k, core).wait_recv()

    barrier = pltpu.get_barrier_semaphore()
    peers = (core, dev_ya, dev_yb, dev_x, dev_xh, up, down)
    for peer in peers:
        pl.semaphore_signal(barrier, inc=1, device_id=peer, device_id_type=MESH)

    own, other = pl.ds(0, R), pl.ds(R, R)

    def local(src, dst, k):
        return pltpu.make_async_copy(src, dst, local_sem.at[k])

    local(mask_hbm, mask.at[:, own], 0).start()

    @pl.when(c == 0)
    def _():
        local(in_hbm, A.at[:, own, :], 1).start()
        local(grad_hbm, B.at[:, own, :], 2).start()

    @pl.when(c == 1)
    def _():
        local(grad_hbm, A.at[:, own, :], 1).start()
        local(in_hbm, B.at[:, own, :], 2).start()

    pl.semaphore_wait(barrier, len(peers))

    km, ka, kb = ids(), ids(), ids()
    m_own, m_other = mask.at[:, own], mask.at[:, other]
    a_other, b_other = A.at[:, other, :], B.at[:, other, :]
    remote(mask_hbm, m_other, km, core).start()

    @pl.when(c == 0)
    def _():
        remote(grad_hbm, a_other, ka, core).start()
        remote(in_hbm, b_other, kb, core).start()

    @pl.when(c == 1)
    def _():
        remote(in_hbm, a_other, ka, core).start()
        remote(grad_hbm, b_other, kb, core).start()

    pending += [(mask_hbm, m_other, km, core), (in_hbm, a_other, ka, core), (in_hbm, b_other, kb, core)]

    local(mask_hbm, m_own, 0).wait()
    local(in_hbm, A.at[:, own, :], 1).wait()
    arrived(m_other, km)
    arrived(a_other, ka)

    dirs = ((1, up), (-1, down))

    def zd(direction, far):
        return (z + NZ + direction * far) % NZ

    class ZRing:
        def __init__(self, W, Rh, Rz, rows, chunks):
            self.W, self.Rh, self.Rz, self.rows, self.chunks = W, Rh, Rz, rows, chunks
            self.k = [[ids(chunks) for _ in range(4)] for _ in range(2)]
            self.half = [pl.ds(0, rows // 2), pl.ds(rows // 2, rows // 2)]

        def at(self, ref, q):
            return ref if q is None else ref.at[q // 2, q % 2]

        def start0(self, q):
            i = 0 if q is None else q
            for n, (direction, to) in enumerate(dirs):
                src = self.at(self.W.at[zd(direction, 4)], q).at[self.half[n]]
                remote(src, self.at(self.Rh.at[n], q), self.k[n][0] + i, to).start()

        def step(self, s, q):
            i = 0 if q is None else q
            for n, (direction, to) in enumerate(dirs):
                w = self.at(self.W.at[zd(direction, 4 - s)], q)
                if s == 1:
                    got = self.at(self.Rh.at[n], q)
                    w = w.at[self.half[n]]
                else:
                    got = self.at(self.Rz.at[n, s - 2], q)
                arrived(got, self.k[n][s - 1] + i)
                w[...] = add(w[...], got[...])
                w = self.at(self.W.at[zd(direction, 4 - s)], q)
                remote(w, self.at(self.Rz.at[n, s - 1], q), self.k[n][s] + i, to).start()

        def finish(self, q):
            i = 0 if q is None else q
            got = []
            for n in range(2):
                g = self.at(self.Rz.at[n, 2], q)
                arrived(g, self.k[n][3] + i)
                got.append(g)
            own = self.at(self.W.at[z], q)
            return (own[...].astype(F32) + got[0][...].astype(F32) + got[1][...].astype(F32)).astype(BF16)

        def drain(self, q):
            i = 0 if q is None else q
            for n, (direction, to) in enumerate(dirs):
                for s in range(4):
                    w = self.at(self.W.at[z], q)
                    w = w.at[self.half[n]] if s == 0 else w
                    remote(w, w, self.k[n][s] + i, to).wait_send()

    class YStage:
        def __init__(self, W, R1, R2, rows):
            self.W, self.R1, self.R2 = W, R1, R2
            self.k1 = [[ids(), ids()], [ids(), ids()]]
            self.k2 = [ids(), ids()]
            h = rows // 2
            self.half = [pl.ds(0, h), pl.ds(h, h)]

        def start(self):
            for s, (d0, to) in enumerate(((ya, dev_ya), (yb, dev_yb))):
                d1 = (3 - ya) if s == 0 else (yb + 1 - 2 * (yb % 2))
                send(self.W.at[d1, :, self.half[s], :], self.R1.at[s, 0], self.k1[s][0], to)
                send(self.W.at[d0, :, self.half[s], :], self.R1.at[s, 1], self.k1[s][1], to)

        def middle(self):
            for s, (d, to) in enumerate(((yb, dev_yb), (ya, dev_ya))):
                arrived(self.R1.at[s, 0], self.k1[s][0])
                w = self.W.at[d, :, self.half[s], :]
                w[...] = add(w[...], self.R1[s, 0])
                send(w, self.R2.at[s], self.k2[s], to)

        def finish(self, out):
            for s in range(2):
                arrived(self.R1.at[s, 1], self.k1[s][1])
                arrived(self.R2.at[s], self.k2[s])
                w = self.W[y, :, self.half[s], :].astype(F32)
                total = w + self.R1[s, 1].astype(F32) + self.R2[s].astype(F32)
                out[:, self.half[s], :] = total.astype(BF16)

    class Pair:
        def __init__(self):
            self.k = ids()

        def start(self, src, got, to):
            self.got = got
            send(src, got, self.k, to)

        def finish(self, own):
            arrived(self.got, self.k)
            return add(own, self.got[...])

    class AllGather:
        def __init__(self, A, rows):
            self.A, self.k = A, [[ids() for _ in range(4)] for _ in range(2)]
            self.half = [pl.ds(0, rows // 2), pl.ds(rows // 2, rows // 2)]

        def piece(self, n, s, index):
            p = self.A.at[index]
            return p.at[self.half[n]] if s == 3 else p

        def step(self, s):
            for n, (direction, to) in enumerate(dirs):
                index = zd(-direction, s)
                if s:
                    p = self.A.at[index]
                    arrived(p, self.k[n][s - 1])
                p = self.piece(n, s, index)
                send(p, p, self.k[n][s], to)

        def finish(self):
            for n, (direction, to) in enumerate(dirs):
                arrived(self.piece(n, 3, zd(-direction, 4)), self.k[n][3])

    fz = ZRing(WF, RFh, RFz, FP, L)
    fy = YStage(FY, RFy1, RFy2, FP)
    fx, fxh, fa = Pair(), Pair(), AllGather(FA, FP)
    gy = YStage(WG, RGy1, RGy2, 8 * T)
    gx = Pair()
    gz = ZRing(GZ, RGh, RGz, GP, 1)
    gxh, ga = Pair(), AllGather(GA, GP)
    k_gp, k_xh, k_xl, k_out = ids(), ids(), ids(), ids()

    def factor(q, carry):
        layer = layer_at[(q % 2) * 4 + q // 2]
        a = A[layer]
        at = a.T
        AT[q] = at
        m = mask[pl.ds(layer, 1), :].astype(F32).astype(BF16)
        am = at * m
        top = dot(am[:R], a) * (1.0 / 65536)
        low = dot(am[R:], a[:, R:]) * (1.0 / 65536)
        for k, (i, j) in enumerate(UPPER):
            if i < 2:
                block = top[i * T : (i + 1) * T, j * T : (j + 1) * T]
            else:
                block = low[(i - 2) * T : (i - 1) * T, (j - 2) * T : (j - 1) * T]
            WF[:, q // 2, q % 2, 16 * k : 16 * (k + 1), :] = block.astype(BF16).reshape(8, 16, T)
        fz.start0(q)
        return carry

    lax.fori_loop(0, L, factor, 0)

    local(in_hbm, B.at[:, own, :], 2).wait()
    arrived(b_other, kb)

    def gradient(q, carry):
        layer = layer_at[(q % 2) * 4 + q // 2]

        @pl.when(c == 0)
        def _():
            g = (dot(AT[q, :R, :], B[layer]) * (1.0 / 256)).astype(BF16)
            for i in range(2):
                for j in range(4):
                    WG[q // 2, q % 2, pl.ds((4 * i + j) * T, T), :] = g[i * T : (i + 1) * T, j * T : (j + 1) * T]

        @pl.when(c == 1)
        def _():
            g = (dot(AT[q], B[layer, :, R:]) * (1.0 / 256)).astype(BF16)
            for i in range(2):
                for j in range(4):
                    WG[q // 2, q % 2, pl.ds((4 * i + j) * T, T), :] = g[j * T : (j + 1) * T, i * T : (i + 1) * T]

        return carry

    lax.fori_loop(0, L, gradient, 0)
    gy.start()

    def loop(f):
        lax.fori_loop(0, L, lambda q, carry: (f(q), carry)[1], 0)

    loop(lambda q: fz.step(1, q))
    gy.middle()
    loop(lambda q: fz.step(2, q))
    loop(lambda q: fz.step(3, q))
    gy.finish(GX)
    gx.start(GX.at[1 - xl], RGx, dev_x)

    def f_last(q):
        FY[q // 2, q % 2] = fz.finish(q)

    loop(f_last)
    fy.start()
    g = gx.finish(GX[xl])
    for k in range(8):
        GZ[:, 16 * k : 16 * (k + 1), :] = g[k * T : (k + 1) * T].reshape(8, 16, T)
    gz.start0(None)
    fy.middle()
    gz.step(1, None)
    fy.finish(FX)
    fx.start(FX.at[1 - xl], RFx, dev_x)
    gz.step(2, None)
    FH[...] = fx.finish(FX[xl])
    fxh.start(FH, RFxh, dev_xh)
    gz.step(3, None)
    FA[z] = fxh.finish(FH[...])
    fa.step(0)
    GH[...] = gz.finish(None)
    gxh.start(GH, RGxh, dev_xh)
    fa.step(1)
    GA[z] = gxh.finish(GH[...])
    ga.step(0)
    fa.step(2)
    ga.step(1)
    fa.step(3)
    ga.step(2)
    fa.finish()
    ga.step(3)

    for k, (i, j) in enumerate(UPPER):
        block = FA[:, 16 * k : 16 * (k + 1), :].reshape(T, T).astype(F32)
        Fm[i * T : (i + 1) * T, j * T : (j + 1) * T] = block
        if i != j:
            Fm[j * T : (j + 1) * T, i * T : (i + 1) * T] = block.T
    eye = (
        lax.broadcasted_iota(jnp.int32, (D, D), 0) == lax.broadcasted_iota(jnp.int32, (D, D), 1)
    ).astype(F32)
    f = Fm[...]
    trace = jnp.sum(jnp.sum(f * eye, axis=0, keepdims=True), axis=1, keepdims=True)
    damped = f + (trace * (0.05 / D)) * eye
    square = jnp.sum(jnp.sum(damped * damped, axis=0, keepdims=True), axis=1, keepdims=True)
    inverse_size = 1.0 / jnp.sqrt(square + 1e-06)
    Pm[...] = eye - damped * inverse_size
    r = split(Pm[...])
    Fm[...] = dot3(r, r)
    r1 = split(Fm[...])
    Qm[...] = dot3(r1, r1)
    Pm[...] = eye + Pm[...] + Fm[...] + dot3(r, r1)
    r2 = split(Qm[...])
    Fm[...] = dot3(r2, r2)
    Pm[...] = Pm[...] + dot3(split(Pm[...]), r2)
    ga.finish()
    send(GA, GAp, k_gp, core)
    r3 = split(Fm[...])
    Pm[...] = (Pm[...] + dot3(split(Pm[...]), r3)) * inverse_size

    arrived(GAp, k_gp)
    xs = split(Pm[...])
    lo, hi = pl.ds(0, R), pl.ds(R, R)

    @pl.when(c == 0)
    def _():
        Xh[...] = xs[0]
        Xl[...] = xs[1]
        remote(Xh, XPh, k_xh, core).start()
        remote(Xl, XPl, k_xl, core).start()
        vh, vl = XPh.at[:, lo], XPl.at[:, lo]
        arrived(vh, k_xh)
        arrived(vl, k_xl)
        out[0, :, lo] = dot3((Xh[...], Xl[...]), (vh[...], vl[...])).astype(BF16)
        remote(Xh, XPh, k_xh, core).wait_send()
        remote(Xl, XPl, k_xl, core).wait_send()
        mine = out.at[0, :, lo]
        remote(mine, mine, k_out, core).start()
        arrived(out.at[0, :, hi], k_out)
        remote(mine, mine, k_out, core).wait_send()

    @pl.when(c == 1)
    def _():
        for i in range(2):
            for j in range(4):
                k = 4 * i + j
                block = GAp[:, 16 * k : 16 * (k + 1), :].reshape(T, T).astype(F32)
                Fm[i * T : (i + 1) * T, j * T : (j + 1) * T] = block
                block = GA[:, 16 * k : 16 * (k + 1), :].reshape(T, T).astype(F32)
                Fm[R + i * T : R + (i + 1) * T, j * T : (j + 1) * T] = block.T
        g = Fm[...].astype(BF16)
        v = split(dot(g, xs[0]) + dot(g, xs[1]))
        Xh[...] = v[0]
        Xl[...] = v[1]
        vh, vl = Xh.at[:, lo], Xl.at[:, lo]
        remote(vh, XPh.at[:, lo], k_xh, core).start()
        remote(vl, XPl.at[:, lo], k_xl, core).start()
        arrived(XPh, k_xh)
        arrived(XPl, k_xl)
        out[0, :, hi] = dot3((XPh[...], XPl[...]), (Xh[:, hi], Xl[:, hi])).astype(BF16)
        remote(vh, XPh.at[:, lo], k_xh, core).wait_send()
        remote(vl, XPl.at[:, lo], k_xl, core).wait_send()
        mine = out.at[0, :, hi]
        remote(mine, mine, k_out, core).start()
        arrived(out.at[0, :, lo], k_out)
        remote(mine, mine, k_out, core).wait_send()

    loop(fz.drain)
    gz.drain(None)
    for src, dst, k, to in pending:
        remote(src, dst, k, to).wait_send()
    assert used[0] <= NSEM


NSEM = 132


def local_step(edge_in, edge_grad, row_mask, layer_at):
    v = pltpu.VMEM
    any_ = pl.BlockSpec(memory_space=pl.ANY)
    return pl.pallas_call(
        kernel,
        out_shape=jax.ShapeDtypeStruct((1, D, D), BF16),
        in_specs=[pl.BlockSpec(memory_space=pltpu.SMEM), any_, any_, any_],
        out_specs=pl.BlockSpec(memory_space=pltpu.VMEM),
        scratch_shapes=[
            v((L, 2 * R), jnp.int32),
            v((L, 2 * R, D), BF16), v((L, 2 * R, D), BF16), v((L, D, 2 * R), BF16),
            v((NZ, 4, 2, FP, T), BF16), v((4, 2, 8 * T, T), BF16),
            v((2, 4, 2, FP // 2, T), BF16), v((2, 3, 4, 2, FP, T), BF16),
            v((4, 2, FP, T), BF16), v((2, 2, 2, FP // 2, T), BF16), v((2, 2, FP // 2, T), BF16),
            v((2, FP, T), BF16), v((FP, T), BF16), v((FP, T), BF16), v((FP, T), BF16), v((NZ, FP, T), BF16),
            v((2, 2, 2, 4 * T, T), BF16), v((2, 2, 4 * T, T), BF16),
            v((2, 8 * T, T), BF16), v((8 * T, T), BF16),
            v((NZ, GP, T), BF16), v((2, GP // 2, T), BF16), v((2, 3, GP, T), BF16),
            v((GP, T), BF16), v((GP, T), BF16), v((NZ, GP, T), BF16), v((NZ, GP, T), BF16),
            v((D, D), F32), v((D, D), F32), v((D, D), F32),
            v((D, D), BF16), v((D, D), BF16), v((D, D), BF16), v((D, D), BF16),
            pltpu.SemaphoreType.DMA((3,)), pltpu.SemaphoreType.DMA((NSEM,)), pltpu.SemaphoreType.DMA((NSEM,)),
        ],
        compiler_params=pltpu.CompilerParams(
            collective_id=0, has_side_effects=True, vmem_limit_bytes=60 * 1024 * 1024
        ),
    )(layer_at, row_mask, edge_in, edge_grad)


def solution(mesh):
    rows = P(None, ("dp", "owner"), None)
    return jax.shard_map(
        local_step, mesh=mesh, in_specs=(rows, rows, P(None, ("dp", "owner")), P()),
        out_specs=P("owner", None, None), check_vma=False,
    )
```

```python
import contextlib
import math

import jax
import jax.numpy as jnp
from jax import lax
from jax.experimental import pallas as pl
from jax.experimental.pallas import tpu as pltpu
from jax.sharding import PartitionSpec as P

MESH = pl.DeviceIdType.MESH
F32 = jnp.float32
BF16 = jnp.bfloat16
L = 8
D = 512
R = 256
NZ = 8
T = 128
UPPER = [(i, j) for i in range(4) for j in range(i, 4)]
NF = len(UPPER)
ZF = 6
YF = NF - ZF
FP, ZP, YP = 16 * NF, 16 * ZF, 16 * YF
GB = 16
GP = 16 * GB


def add(a, b):
    return (a.astype(F32) + b.astype(F32)).astype(BF16)


def split(x):
    hi = x.astype(BF16)
    return hi, (x - hi.astype(F32)).astype(BF16)


def dot(a, b):
    return lax.dot_general(a, b, (((1,), (0,)), ((), ())), preferred_element_type=F32)


def dot3(a, b):
    (ah, al), (bh, bl) = a, b
    return dot(ah, bh) + (dot(ah, bl) + dot(al, bh))


def kernel(
    layer_at, mask_hbm, in_hbm, grad_hbm, out,
    mask, rows_in, rows_grad, dummy,
    WZ, RZ, VZ, RZr, RZd, XZ, XZr,
    WY0, RY0r, RY0d, WY1, RY1r, RY1d, XY, XYr, UY, RU, HY, HYr, FA,
    WX, RX, VX, RXr, RXd, YX, UG, RUG, HG, HGr, GA,
    Fm, Pm, Qm, Gm, X, Xp, local_sem, send_sem, recv_sem,
):
    dp, ow = lax.axis_index("dp"), lax.axis_index("owner")
    z, xh, c = dp // 4, (dp // 2) % 2, dp % 2
    xl, y = ow // 4, ow % 4

    def dev(z=z, xh=xh, c=c, xl=xl, y=y):
        return (z * 4 + xh * 2 + c, xl * 4 + y)

    ya = y + 1 - 2 * (y % 2)
    yb = 3 - y
    yo = (y + 2) % 4
    core = dev(c=1 - c)
    dev_ya, dev_yb = dev(y=ya), dev(y=yb)
    dev_x, dev_x2, dev_xh = dev(xl=1 - xl), dev(xl=1 - xl, xh=1 - xh), dev(xh=1 - xh)
    up, down = dev(z=(z + 1) % NZ), dev(z=(z + NZ - 1) % NZ)

    used = [0]
    groups, groupsG = [], []

    def ids():
        used[0] += 1
        return used[0] - 1

    def remote(src, dst, k, to, g=0):
        return pltpu.make_async_remote_copy(
            src_ref=src, dst_ref=dst, send_sem=send_sem.at[g], recv_sem=recv_sem.at[k],
            device_id=to, device_id_type=MESH,
        )

    def send(src, dst, k, to):
        size = math.prod(src.shape) * src.dtype.itemsize
        if not groups or groups[-1] + size > SENT:
            groups.append(0)
        groups[-1] += size
        remote(src, dst, k, to, len(groups) - 1).start()

    def sent(groups):
        for g, size in enumerate(groups):
            ref = dummy.at[pl.ds(0, size // (2 * D))]
            pltpu.make_async_copy(ref, ref, send_sem.at[g]).wait()
        assert len(groups) <= LAST, len(groups)

    def arrived(dst, k):
        remote(dst, dst, k, core).wait_recv()

    @contextlib.contextmanager
    def stage(name):
        with jax.named_scope(name):
            yield
        if FENCE:
            pl.delay(1)

    barrier = pltpu.get_barrier_semaphore()
    column = [dev(z=(z + far) % NZ) for far in (4, 3, 5, 2, 6, 1, 7)]
    peers = (core, dev_ya, dev_yb, dev_x, dev_x2, dev_xh, *column)
    for peer in peers:
        pl.semaphore_signal(barrier, inc=1, device_id=peer, device_id_type=MESH)

    own, other = pl.ds(0, R), pl.ds(R, R)
    loads = ((mask_hbm, mask.at[:, own]), (in_hbm, rows_in.at[:, own, :]), (grad_hbm, rows_grad.at[:, own, :]))
    gets = [(mask_hbm, mask.at[:, other]), (in_hbm, rows_in.at[:, other, :]), (grad_hbm, rows_grad.at[:, other, :])]
    gets = [(src, dst, ids(), LAST + i) for i, (src, dst) in enumerate(gets)]
    for i, (src, dst) in enumerate(loads):
        pltpu.make_async_copy(src, dst, local_sem.at[i]).start()
    with stage("barrier"):
        pl.semaphore_wait(barrier, len(peers))
        for src, dst, k, g in gets:
            remote(src, dst, k, core, g).start()

    def loaded(i):
        src, dst = loads[i]
        pltpu.make_async_copy(src, dst, local_sem.at[i]).wait()
        arrived(gets[i][1], gets[i][2])

    with stage("waitA"):
        loaded(0)
        loaded(1)

    dirs = ((1, up), (-1, down))

    def zd(direction, far):
        return (z + NZ + direction * far) % NZ

    class ZRing:
        def __init__(self, W, Rz, rows, chunks):
            self.W, self.Rz = W, Rz
            self.k = [[ids() for _ in range(chunks)] for _ in range(4)]
            self.half = [pl.ds(0, rows // 2), pl.ds(rows // 2, rows // 2)]

        def go(self, n, s, q, half=None):
            w, r = self.W.at[zd(dirs[n][0], 4 - s), q], self.Rz.at[s, q, n]
            if half is not None:
                w, r = w.at[:, half, :], r.at[:, half, :]
            send(w, r, self.k[s][q], dirs[n][1])

        def start(self, q=0):
            for n in range(2):
                self.go(n, 0, q, self.half[n])
            for n in range(2):
                self.go(n, 1, q, self.half[1 - n])

        def step(self, s, q=0):
            arrived(self.Rz.at[s - 1, q, 0] if s == 1 else self.Rz.at[s - 1, q], self.k[s - 1][q])
            for n in range(2):
                d = zd(dirs[n][0], 4 - s)
                if s == 1:
                    h = self.half[n]
                    self.W[d, q, :, h, :] = add(self.W[d, q, :, h, :], self.Rz[0, q, n, :, h, :])
                    self.go(n, 1, q, h)
                else:
                    self.W[d, q] = add(self.W[d, q], self.Rz[s - 1, q, n])
                    self.go(n, s, q)

        def finish(self, q=0):
            arrived(self.Rz.at[3, q], self.k[3][q])
            mine = self.W[z, q].astype(F32)
            return (mine + (self.Rz[3, q, 0].astype(F32) + self.Rz[3, q, 1].astype(F32))).astype(BF16)

    class YStage:
        def __init__(self, W, Rr, Rd, rows):
            self.W, self.Rr, self.Rd = W, Rr, Rd
            self.kr, self.kd = ids(), ids()
            h = rows // 2
            self.half = [pl.ds(0, h), pl.ds(h, h)]

        def relay(self):
            for s, to in enumerate((dev_ya, dev_yb)):
                send(self.W.at[yo, :, self.half[s], :], self.Rr.at[s], self.kr, to)

        def direct(self, s):
            d, to = ((ya, dev_ya), (yb, dev_yb))[s]
            send(self.W.at[d, :, self.half[s], :], self.Rd.at[0, s], self.kd, to)

        def start(self):
            self.relay()
            self.direct(0)
            self.direct(1)

        def middle(self):
            arrived(self.Rr, self.kr)
            for s, (d, to) in enumerate(((yb, dev_yb), (ya, dev_ya))):
                h = self.half[s]
                self.W[d, :, h, :] = add(self.W[d, :, h, :], self.Rr[s])
                send(self.W.at[d, :, h, :], self.Rd.at[1, s], self.kd, to)

        def finish(self, out):
            arrived(self.Rd, self.kd)
            for s in range(2):
                h = self.half[s]
                total = self.W[y, :, h, :].astype(F32) + (self.Rd[0, s].astype(F32) + self.Rd[1, s].astype(F32))
                out[:, h, :] = total.astype(BF16)

    class AllGather:
        def __init__(self, A, rows):
            self.A, self.k = A, [ids() for _ in range(4)]
            self.half = [pl.ds(0, rows // 2), pl.ds(rows // 2, rows // 2)]

        def step(self, s):
            if s:
                arrived(self.A.at[pl.ds(0, 2)], self.k[s - 1])
            for n, (direction, to) in enumerate(dirs):
                p = self.A.at[zd(-direction, s)]
                p = p.at[self.half[n]] if s == 3 else p
                send(p, p, self.k[s], to)

        def finish(self):
            arrived(self.A.at[0], self.k[3])

    order = (yo, ya, yb, y)
    fz = ZRing(WZ, RZ, ZP, 8)
    fzy = YStage(VZ, RZr, RZd, ZP)
    fy = (YStage(WY0, RY0r, RY0d, YF * T), YStage(WY1, RY1r, RY1d, YF * T))
    fyz = ZRing(UY, RU, YP, 1)
    fa = (AllGather(FA.at[0], FP), AllGather(FA.at[1], FP))
    gxy = YStage(VX, RXr, RXd, GB * T)
    gz = ZRing(UG, RUG, GP, 1)
    k_fx = [ids() for _ in range(2)]
    k_gx = [ids() for _ in range(4)]
    k_xz, k_fh, k_gh, k_ga = (ids() for _ in range(4))
    k_fp, k_gp, k_x, k_out = (ids() for _ in range(4))

    def pieces(ref, m, first, f, n):
        for k in range(n):
            ref[:, 0, m, 16 * (first + k) : 16 * (first + k + 1), :] = f[k * T : (k + 1) * T].reshape(8, 16, T)

    def factor(i, x):
        f, t = i // 4, i % 4
        d = order[t]
        layer = layer_at[x * 4 + d]
        a = (rows_in, rows_grad)[f][layer]
        m = mask[pl.ds(layer, 1), :].astype(F32).astype(BF16)
        am = a.T * m
        top = dot(am[:R], a) * (1.0 / 65536)
        low = dot(am[R:], a[:, R:]) * (1.0 / 65536)
        for k, (p, q) in enumerate(UPPER):
            if p < 2:
                block = top[p * T : (p + 1) * T, q * T : (q + 1) * T].astype(BF16)
            else:
                block = low[(p - 2) * T : (p - 1) * T, (q - 2) * T : (q - 1) * T].astype(BF16)
            if k < ZF:
                WZ[:, i, x, 16 * k : 16 * (k + 1), :] = block.reshape(8, 16, T)
            else:
                (WY0, WY1)[f][d, x, (k - ZF) * T : (k - ZF + 1) * T, :] = block

    def gradient(t, x):
        d = order[t]
        layer = layer_at[x * 4 + d]
        g = (dot(rows_in[layer].T, rows_grad[layer]) * (1.0 / 256)).astype(BF16)
        for k in range(GB):
            p, q = k // 4, k % 4
            block = g[p * T : (p + 1) * T, q * T : (q + 1) * T]
            WX[x, d, k * T : (k + 1) * T, :] = block

    def both(f, t):
        lax.fori_loop(0, 2, lambda x, carry: (f(t, x), carry)[1], 0)

    def leave(ystage, t):
        if t == 0:
            ystage.relay()
        elif t < 3:
            ystage.direct(t - 1)

    halves = ((pl.ds(0, GB * T // 2), dev_x), (pl.ds(GB * T // 2, GB * T // 2), dev_x2))

    @pl.when(c == 1)
    def _():
        for i in range(8):
            f, t = i // 4, i % 4
            with stage(f"factor{i}"):
                if i == 4:
                    loaded(2)
                both(factor, i)
                fz.start(i)
                leave(fy[f], t)
            if i == 4:
                with stage("fy0mid"):
                    fy[0].middle()
            if i >= 3:
                with stage("fz1"):
                    fz.step(1, i - 3)

        def fx(f):
            with stage("fyfin"):
                fy[f].finish(XY.at[f])
                send(XY.at[f, 1 - xl], XYr.at[f], k_fx[f], dev_x)

        with stage("fz1"):
            fz.step(1, 5)
        fx(0)
        with stage("fy1mid"):
            fy[1].middle()
        for i in range(6, 8):
            with stage("fz1"):
                fz.step(1, i)
        for i in range(6):
            with stage("fz2"):
                fz.step(2, i)
        fx(1)
        for i in range(6, 8):
            with stage("fz2"):
                fz.step(2, i)
        for i in range(4):
            with stage("fz3"):
                fz.step(3, i)
        with stage("fxfin"):
            for f in range(2):
                arrived(XYr.at[f], k_fx[f])
                pieces(UY, f, 0, add(XY[f, xl], XYr[f]), YF)
            fyz.start()
        for i in range(4, 8):
            with stage("fz3"):
                fz.step(3, i)
        for t in range(4):
            with stage("fzfin"):
                for f in range(2):
                    v = fz.finish(4 * f + t)
                    for x in range(2):
                        VZ[order[t], 2 * x + f] = v[x]
                leave(fzy, t)
        with stage("fyz1"):
            fyz.step(1)
        with stage("fzymid"):
            fzy.middle()
        with stage("fyz2"):
            fyz.step(2)
        with stage("fzyfin"):
            fzy.finish(XZ)
            theirs = XZ.at[pl.ds(2 * (1 - xl), 2)]
            send(theirs, XZr.at[0], k_xz, dev_x)
            send(theirs, XZr.at[1], k_xz, dev_x2)
            send(XZ.at[pl.ds(2 * xl, 2)], XZr.at[2], k_xz, dev_xh)
        with stage("fyz3"):
            fyz.step(3)
        with stage("fyzfin"):
            HY[...] = fyz.finish()
            send(HY, HYr, k_fh, dev_xh)
        with stage("fxm"):
            arrived(XZr, k_xz)
            near = XZr[0].astype(F32) + XZr[1].astype(F32)
            FA[:, z, :ZP, :] = ((XZ[pl.ds(2 * xl, 2)].astype(F32) + XZr[2].astype(F32)) + near).astype(BF16)
        with stage("fhfin"):
            arrived(HYr, k_fh)
            FA[:, z, ZP:, :] = add(HY[...], HYr[...])
            fa[0].step(0)
            fa[1].step(0)
        for s in range(1, 4):
            with stage(f"fa{s}"):
                fa[0].step(s)
                fa[1].step(s)
        with stage("fafin"):
            fa[0].finish()
            send(FA.at[0], FA.at[0], k_fp, core)
            fa[1].finish()

    @pl.when(c == 0)
    def _():
        kept, groups[:] = list(groups), []
        with stage("waitB"):
            loaded(2)
        for t in range(4):
            with stage("grad"):
                both(gradient, t)
                d = order[t]
                for h, to in halves:
                    send(WX.at[1 - xl, d, h, :], RX.at[d, h, :], k_gx[t], to)
        for t in range(4):
            with stage("gx"):
                d = order[t]
                arrived(RX.at[d], k_gx[t])
                VX[d, 0] = add(WX[xl, d], RX[d])
                leave(gxy, t)
        with stage("gxymid"):
            gxy.middle()
        with stage("gxyfin"):
            gxy.finish(YX)
            pieces(UG, 0, 0, YX[0], GB)
            gz.start()
        for s in range(1, 4):
            with stage(f"gz{s}"):
                gz.step(s)
        with stage("gzfin"):
            HG[...] = gz.finish()[0]
            send(HG, HGr, k_gh, dev_xh)
        with stage("ghfin"):
            arrived(HGr, k_gh)
            GA[z] = add(HG[...], HGr[...])
            for to in column:
                send(GA.at[z], GA.at[z], k_ga, to)
        with stage("waitF"):
            arrived(FA.at[0], k_fp)
        groupsG.extend(groups)
        groups[:] = kept

    with stage("damp"):
        for k, (p, q) in enumerate(UPPER):
            block = FA[c, :, 16 * k : 16 * (k + 1), :].reshape(T, T).astype(F32)
            Fm[p * T : (p + 1) * T, q * T : (q + 1) * T] = block
            if p != q:
                Fm[q * T : (q + 1) * T, p * T : (p + 1) * T] = block.T
        eye = (
            lax.broadcasted_iota(jnp.int32, (D, D), 0) == lax.broadcasted_iota(jnp.int32, (D, D), 1)
        ).astype(F32)
        f = Fm[...]
        trace = jnp.sum(jnp.sum(f * eye, axis=0, keepdims=True), axis=1, keepdims=True)
        damped = f + (trace * (0.05 / D)) * eye
        square = jnp.sum(jnp.sum(damped * damped, axis=0, keepdims=True), axis=1, keepdims=True)
        inverse_size = 1.0 / jnp.sqrt(square + 1e-06)
        Pm[...] = eye - damped * inverse_size

    with stage("ns1"):
        r = split(Pm[...])
        Fm[...] = dot3(r, r)
    with stage("ns2"):
        r1 = split(Fm[...])
        Qm[...] = dot3(r1, r1)

    with stage("ns3"):
        Pm[...] = eye + Pm[...] + Fm[...] + dot3(r, r1)

    with stage("ns4"):
        r2 = split(Qm[...])
        Fm[...] = dot3(r2, r2)
        Pm[...] = Pm[...] + dot3(split(Pm[...]), r2)

    with stage("ns5"):
        r3 = split(Fm[...])
        X[0], X[1] = split((Pm[...] + dot3(split(Pm[...]), r3)) * inverse_size)

    lo, hi = pl.ds(0, R), pl.ds(R, R)

    def gather():
        for k in range(GB):
            p, q = k // 4, k % 4
            Gm[p * T : (p + 1) * T, q * T : (q + 1) * T] = GA[:, 16 * k : 16 * (k + 1), :].reshape(T, T)

    out_lo, out_hi = out.at[0, :, lo], out.at[0, :, hi]

    @pl.when(c == 1)
    def _():
        remote(X.at[:, :, lo], Xp.at[:, :, lo], k_x, core, LAST + 3).start()
        with stage("gafin"):
            arrived(GA, k_gp)
        with stage("gather"):
            gather()
            right = split(dot(Gm[...], X[0, :, hi]) + dot(Gm[...], X[1, :, hi]))
        with stage("waitX"):
            arrived(Xp, k_x)
        with stage("last"):
            out[0, :, hi] = dot3((Xp[0], Xp[1]), right).astype(BF16)
            remote(out_hi, out_hi, k_out, core, LAST + 4).start()
            remote(X.at[:, :, lo], Xp.at[:, :, lo], k_x, core, LAST + 3).wait_send()
            sent(groups)

    @pl.when(c == 0)
    def _():
        remote(X, Xp, k_x, core, LAST + 3).start()
        with stage("gafin"):
            arrived(GA.at[pl.ds(0, NZ - 1)], k_ga)
            remote(GA, GA, k_gp, core, LAST + 5).start()
        with stage("gather"):
            gather()
            left = split(dot(X[0], Gm[...]) + dot(X[1], Gm[...]))
        with stage("waitX"):
            arrived(Xp.at[:, :, lo], k_x)
        with stage("last"):
            out[0, :, lo] = dot3(left, (Xp[0, :, lo], Xp[1, :, lo])).astype(BF16)
            remote(out_lo, out_lo, k_out, core, LAST + 4).start()
            remote(X, Xp, k_x, core, LAST + 3).wait_send()
            remote(GA, GA, k_gp, core, LAST + 5).wait_send()
            sent(groupsG)

    with stage("waitO"):
        arrived(out_lo, k_out)
        remote(out_lo, out_lo, k_out, core, LAST + 4).wait_send()
        for src, dst, k, g in gets:
            remote(src, dst, k, core, g).wait_send()
    assert used[0] == NSEM, used[0]


FENCE = True
SENT = 2 * 1024 * 1024
NSEM = 73
LAST = 6
NSEND = LAST + 6


def local_step(edge_in, edge_grad, row_mask, layer_at):
    def v(*shape, dtype=BF16):
        return pltpu.VMEM(shape, dtype)

    def ystage(m, rows):
        return [v(4, m, rows, T), v(2, m, rows // 2, T), v(2, 2, m, rows // 2, T)]

    def zring(chunks, m, rows):
        return [v(NZ, chunks, m, rows, T), v(4, chunks, 2, m, rows, T)]

    yf, gb = YF * T, GB * T
    any_ = pl.BlockSpec(memory_space=pl.ANY)
    return pl.pallas_call(
        kernel,
        out_shape=jax.ShapeDtypeStruct((1, D, D), BF16),
        in_specs=[pl.BlockSpec(memory_space=pltpu.SMEM), any_, any_, any_],
        out_specs=pl.BlockSpec(memory_space=pltpu.VMEM),
        scratch_shapes=[
            v(L, 2 * R, dtype=jnp.int32), v(L, 2 * R, D), v(L, 2 * R, D), v(SENT // (2 * D), D),
            *zring(8, 2, ZP), *ystage(4, ZP), v(4, ZP, T), v(3, 2, ZP, T),
            *ystage(2, yf), *ystage(2, yf), v(2, 2, yf, T), v(2, yf, T), *zring(1, 2, YP), v(2, YP, T), v(2, YP, T),
            v(2, NZ, FP, T),
            v(2, 4, gb, T), v(4, gb, T), *ystage(1, gb), v(1, gb, T),
            *zring(1, 1, GP), v(GP, T), v(GP, T), v(NZ, GP, T),
            v(D, D, dtype=F32), v(D, D, dtype=F32), v(D, D, dtype=F32), v(D, D), v(2, D, D), v(2, D, D),
            pltpu.SemaphoreType.DMA((3,)), pltpu.SemaphoreType.DMA((NSEND,)), pltpu.SemaphoreType.DMA((NSEM,)),
        ],
        compiler_params=pltpu.CompilerParams(
            collective_id=0, has_side_effects=True, vmem_limit_bytes=60 * 1024 * 1024
        ),
    )(layer_at, row_mask, edge_in, edge_grad)


def solution(mesh):
    rows = P(None, ("dp", "owner"), None)
    return jax.shard_map(
        local_step, mesh=mesh, in_specs=(rows, rows, P(None, ("dp", "owner")), P()),
        out_specs=P("owner", None, None), check_vma=False,
    )
```

```python
import contextlib
import math

import jax
import jax.numpy as jnp
from jax import lax
from jax.experimental import pallas as pl
from jax.experimental.pallas import tpu as pltpu
from jax.sharding import PartitionSpec as P

MESH = pl.DeviceIdType.MESH
F32 = jnp.float32
BF16 = jnp.bfloat16
L = 8
D = 512
R = 256
NZ = 8
T = 128
UPPER = [(i, j) for i in range(4) for j in range(i, 4)]
NF = len(UPPER)
ZF = 7
YF = NF - ZF
ZP, YP = 16 * ZF, 16 * YF
GB = 16
HB = 4
XB = GB - HB
GP = 16 * GB


def add(a, b):
    return (a.astype(F32) + b.astype(F32)).astype(BF16)


def split(x):
    hi = x.astype(BF16)
    return hi, (x - hi.astype(F32)).astype(BF16)


def dot(a, b):
    return lax.dot_general(a, b, (((1,), (0,)), ((), ())), preferred_element_type=F32)


def dot3(a, b):
    (ah, al), (bh, bl) = a, b
    return dot(ah, bh) + (dot(ah, bl) + dot(al, bh))


def kernel(
    layer_at, mask_hbm, in_hbm, grad_hbm, out,
    mask, rows_in, rows_grad, dummy,
    WZ, RZ, VZ, RZr, RZd, XZ, XZr,
    WY0, RY0r, RY0d, WY1, RY1r, RY1d, XY, XYr, UY, RUr, RUd, HY, HYr, FZ, FY,
    WG, RGr, RGd, XG, XGr, WX, RX, VX, RXr, RXd, YX, UG, RUGr, RUGd, HG, HGr, GA,
    Fm, Pm, Qm, Gm, X, Xp, mine, local_sem, send_sem, recv_sem,
):
    dp, ow = lax.axis_index("dp"), lax.axis_index("owner")
    z, xh, c = dp // 4, (dp // 2) % 2, dp % 2
    xl, y = ow // 4, ow % 4

    def dev(z=z, xh=xh, c=c, xl=xl, y=y):
        return (z * 4 + xh * 2 + c, xl * 4 + y)

    ya = y + 1 - 2 * (y % 2)
    yb = 3 - y
    yo = (y + 2) % 4
    core = dev(c=1 - c)
    dev_ya, dev_yb = dev(y=ya), dev(y=yb)
    dev_x, dev_x2, dev_xh = dev(xl=1 - xl), dev(xl=1 - xl, xh=1 - xh), dev(xh=1 - xh)
    up, down = dev(z=(z + 1) % NZ), dev(z=(z + NZ - 1) % NZ)

    used = [0]
    groups, groupsG = [], []

    def ids():
        used[0] += 1
        return used[0] - 1

    def remote(src, dst, k, to, g=0):
        return pltpu.make_async_remote_copy(
            src_ref=src, dst_ref=dst, send_sem=send_sem.at[g], recv_sem=recv_sem.at[k],
            device_id=to, device_id_type=MESH,
        )

    def send(src, dst, k, to):
        size = math.prod(src.shape) * src.dtype.itemsize
        if not groups or groups[-1] + size > SENT:
            groups.append(0)
        groups[-1] += size
        remote(src, dst, k, to, len(groups) - 1).start()

    def sent(groups):
        for g, size in enumerate(groups):
            ref = dummy.at[pl.ds(0, size // (2 * D))]
            pltpu.make_async_copy(ref, ref, send_sem.at[g]).wait()
        assert len(groups) <= LAST, len(groups)

    def arrived(dst, k):
        remote(dst, dst, k, core).wait_recv()

    @contextlib.contextmanager
    def stage(name):
        with jax.named_scope(name):
            yield
        if FENCE:
            pl.delay(1)

    barrier = pltpu.get_barrier_semaphore()
    up2, down2 = dev(z=(z + 2) % NZ), dev(z=(z + NZ - 2) % NZ)
    peers = (core, dev_ya, dev_yb, dev_x, dev_x2, dev_xh, up, down, up2, down2)
    for peer in peers:
        pl.semaphore_signal(barrier, inc=1, device_id=peer, device_id_type=MESH)

    own, other = pl.ds(0, R), pl.ds(R, R)
    loads = ((mask_hbm, mask.at[:, own]), (in_hbm, rows_in.at[:, own, :]), (grad_hbm, rows_grad.at[:, own, :]))
    gets = [(mask_hbm, mask.at[:, other]), (in_hbm, rows_in.at[:, other, :]), (grad_hbm, rows_grad.at[:, other, :])]
    gets = [(src, dst, ids(), LAST + i) for i, (src, dst) in enumerate(gets)]
    for i, (src, dst) in enumerate(loads):
        pltpu.make_async_copy(src, dst, local_sem.at[i]).start()
    with stage("barrier"):
        pl.semaphore_wait(barrier, len(peers))
        for src, dst, k, g in gets:
            remote(src, dst, k, core, g).start()

    def loaded(i):
        src, dst = loads[i]
        pltpu.make_async_copy(src, dst, local_sem.at[i]).wait()
        arrived(gets[i][1], gets[i][2])

    with stage("waitA"):
        loaded(0)
        loaded(1)

    dirs = ((1, up, up2), (-1, down, down2))

    def zd(direction, far):
        return (z + NZ + direction * far) % NZ

    class ZRing:
        def __init__(self, W, Rz, rows, chunks):
            self.W, self.Rz = W, Rz
            self.k = [[ids() for _ in range(chunks)] for _ in range(4)]
            self.half = [pl.ds(0, rows // 2), pl.ds(rows // 2, rows // 2)]

        def go(self, n, s, q, half=None):
            w, r = self.W.at[zd(dirs[n][0], 4 - s), q], self.Rz.at[s, q, n]
            if half is not None:
                w, r = w.at[:, half, :], r.at[:, half, :]
            send(w, r, self.k[s][q], dirs[n][1])

        def start(self, q=0):
            for n in range(2):
                self.go(n, 0, q, self.half[n])
            for n in range(2):
                self.go(n, 1, q, self.half[1 - n])

        def step(self, s, q=0):
            arrived(self.Rz.at[s - 1, q, 0] if s == 1 else self.Rz.at[s - 1, q], self.k[s - 1][q])
            for n in range(2):
                d = zd(dirs[n][0], 4 - s)
                if s == 1:
                    h = self.half[n]
                    self.W[d, q, :, h, :] = add(self.W[d, q, :, h, :], self.Rz[0, q, n, :, h, :])
                    self.go(n, 1, q, h)
                else:
                    self.W[d, q] = add(self.W[d, q], self.Rz[s - 1, q, n])
                    self.go(n, s, q)

        def finish(self, q=0):
            arrived(self.Rz.at[3, q], self.k[3][q])
            mine = self.W[z, q].astype(F32)
            return (mine + (self.Rz[3, q, 0].astype(F32) + self.Rz[3, q, 1].astype(F32))).astype(BF16)

    class YStage:
        def __init__(self, W, Rr, Rd, rows):
            self.W, self.Rr, self.Rd = W, Rr, Rd
            self.kr, self.kd = ids(), ids()
            h = rows // 2
            self.half = [pl.ds(0, h), pl.ds(h, h)]

        def relay(self):
            for s, to in enumerate((dev_ya, dev_yb)):
                send(self.W.at[yo, :, self.half[s], :], self.Rr.at[s], self.kr, to)

        def direct(self, s):
            d, to = ((ya, dev_ya), (yb, dev_yb))[s]
            send(self.W.at[d, :, self.half[s], :], self.Rd.at[0, s], self.kd, to)

        def start(self):
            self.relay()
            self.direct(0)
            self.direct(1)

        def middle(self):
            arrived(self.Rr, self.kr)
            for s, (d, to) in enumerate(((yb, dev_yb), (ya, dev_ya))):
                h = self.half[s]
                self.W[d, :, h, :] = add(self.W[d, :, h, :], self.Rr[s])
                send(self.W.at[d, :, h, :], self.Rd.at[1, s], self.kd, to)

        def finish(self, out):
            arrived(self.Rd, self.kd)
            for s in range(2):
                h = self.half[s]
                total = self.W[y, :, h, :].astype(F32) + (self.Rd[0, s].astype(F32) + self.Rd[1, s].astype(F32))
                out[:, h, :] = total.astype(BF16)

    class ZPair:
        def __init__(self, W, Rr, Rd, rows):
            self.W, self.Rr, self.Rd, self.kr, self.kd = W, Rr, Rd, ids(), ids()
            self.half = [pl.ds(0, rows // 2), pl.ds(rows // 2, rows // 2)]

        def start(self):
            W, Rr = self.W, self.Rr
            for n, (direction, to, to2) in enumerate(dirs):
                send(W.at[zd(direction, 3), 0], Rr.at[n], self.kr, to)
                h = self.half[n]
                send(W.at[zd(direction, 4), 0, :, h, :], Rr.at[2, :, h, :], self.kr, to2)
            for n, (direction, to, to2) in enumerate(dirs):
                send(W.at[zd(direction, 1), 0], self.Rd.at[n], self.kd, to)

        def middle(self):
            W, Rr = self.W, self.Rr
            arrived(Rr, self.kr)
            for n, (direction, to, to2) in enumerate(dirs):
                d = zd(direction, 2)
                near, far = self.half[1 - n], self.half[n]
                W[d, 0, :, near, :] = add(W[d, 0, :, near, :], Rr[n, :, near, :])
                both = Rr[n, :, far, :].astype(F32) + Rr[2, :, far, :].astype(F32)
                W[d, 0, :, far, :] = (W[d, 0, :, far, :].astype(F32) + both).astype(BF16)
                send(W.at[d, 0], self.Rd.at[2 + n], self.kd, to2)

        def finish(self):
            Rd = self.Rd
            arrived(Rd, self.kd)
            near = Rd[0].astype(F32) + Rd[1].astype(F32)
            far = Rd[2].astype(F32) + Rd[3].astype(F32)
            return ((self.W[z, 0].astype(F32) + near) + far).astype(BF16)

    class AllGather:
        def __init__(self, A, rows):
            self.A, self.k = A, [ids() for _ in range(3)]
            self.half = [pl.ds(0, rows // 2), pl.ds(rows // 2, rows // 2)]

        def start(self):
            p = self.A.at[z]
            for direction, to, to2 in dirs:
                send(p, p, self.k[0], to)
            for direction, to, to2 in dirs:
                send(p, p, self.k[1], to2)

        def relay(self):
            arrived(self.A.at[pl.ds(0, 2)], self.k[1])
            for n, (direction, to, to2) in enumerate(dirs):
                p = self.A.at[zd(-direction, 2)]
                send(p, p, self.k[2], to)
            for n, (direction, to, to2) in enumerate(dirs):
                p = self.A.at[zd(-direction, 2), self.half[n], :]
                send(p, p, self.k[2], to2)

        def finish(self):
            arrived(self.A.at[pl.ds(0, 2)], self.k[0])
            arrived(self.A.at[pl.ds(0, 3)], self.k[2])

    order = (yo, ya, yb, y)
    fz = ZRing(WZ, RZ, ZP, 8)
    fzy = YStage(VZ, RZr, RZd, ZP)
    fy = (YStage(WY0, RY0r, RY0d, YF * T), YStage(WY1, RY1r, RY1d, YF * T))
    fyz = ZPair(UY, RUr, RUd, YP)
    faz = (AllGather(FZ.at[0], ZP), AllGather(FZ.at[1], ZP))
    fay = (AllGather(FY.at[0], YP), AllGather(FY.at[1], YP))
    gy = YStage(WG, RGr, RGd, HB * T)
    gxy = YStage(VX, RXr, RXd, XB * T)
    gz = ZPair(UG, RUGr, RUGd, GP)
    ga = AllGather(GA, GP)
    k_fx = [ids() for _ in range(2)]
    k_gx = [ids() for _ in range(4)]
    k_xz, k_fh, k_gh, k_xg = (ids() for _ in range(4))
    k_fpz, k_fpy, k_gp, k_x, k_out = (ids() for _ in range(5))

    def pieces(ref, m, first, f, n):
        for k in range(n):
            ref[:, 0, m, 16 * (first + k) : 16 * (first + k + 1), :] = f[k * T : (k + 1) * T].reshape(8, 16, T)

    def factor(i, x):
        f, t = i // 4, i % 4
        d = order[t]
        layer = layer_at[x * 4 + d]
        a = (rows_in, rows_grad)[f][layer]
        m = mask[pl.ds(layer, 1), :].astype(F32).astype(BF16)
        am = a.T * m
        top = dot(am[:R], a) * (1.0 / 65536)
        low = dot(am[R:], a[:, R:]) * (1.0 / 65536)
        for k, (p, q) in enumerate(UPPER):
            if p < 2:
                block = top[p * T : (p + 1) * T, q * T : (q + 1) * T].astype(BF16)
            else:
                block = low[(p - 2) * T : (p - 1) * T, (q - 2) * T : (q - 1) * T].astype(BF16)
            if k < ZF:
                WZ[:, i, x, 16 * k : 16 * (k + 1), :] = block.reshape(8, 16, T)
            else:
                (WY0, WY1)[f][d, x, (k - ZF) * T : (k - ZF + 1) * T, :] = block

    def gradient(t, x):
        d = order[t]
        layer = layer_at[x * 4 + d]
        g = (dot(rows_in[layer].T, rows_grad[layer]) * (1.0 / 256)).astype(BF16)
        for k in range(GB):
            p, q = k // 4, k % 4
            block = g[p * T : (p + 1) * T, q * T : (q + 1) * T]
            if k < HB:
                WG[d, x, k * T : (k + 1) * T, :] = block
            else:
                WX[x, d, (k - HB) * T : (k - HB + 1) * T, :] = block

    def both(f, t):
        lax.fori_loop(0, 2, lambda x, carry: (f(t, x), carry)[1], 0)

    def leave(ystage, t):
        if t == 0:
            ystage.relay()
        elif t < 3:
            ystage.direct(t - 1)

    def halves(rows):
        return (pl.ds(0, rows // 2), dev_x), (pl.ds(rows // 2, rows // 2), dev_x2)


    @pl.when(c == 1)
    def _():
        def fx(f):
            with stage("fyfin"):
                fy[f].finish(XY.at[f])
                for h, to in halves(YF * T):
                    send(XY.at[f, 1 - xl, h, :], XYr.at[f, h, :], k_fx[f], to)

        for i in range(8 + 3 * LAG):
            if i < 8:
                f, t = i // 4, i % 4
                with stage(f"factor{i}"):
                    if i == 4:
                        loaded(2)
                    both(factor, i)
                    fz.start(i)
                    leave(fy[f], t)
            for s in (3, 2, 1):
                if 0 <= i - s * LAG < 8:
                    with stage(f"fz{s}"):
                        fz.step(s, i - s * LAG)
            if i == 4:
                with stage("fy0mid"):
                    fy[0].middle()
            if i == 8:
                with stage("fy1mid"):
                    fy[1].middle()
            if i in AT_FX:
                fx(AT_FX.index(i))
        with stage("fxfin"):
            for f in range(2):
                arrived(XYr.at[f], k_fx[f])
                pieces(UY, f, 0, add(XY[f, xl], XYr[f]), YF)
            fyz.start()
        for t in range(4):
            with stage("fzfin"):
                for f in range(2):
                    v = fz.finish(4 * f + t)
                    for x in range(2):
                        VZ[order[t], 2 * x + f] = v[x]
                leave(fzy, t)
        with stage("fyzmid"):
            fyz.middle()
        with stage("fzymid"):
            fzy.middle()
        with stage("fyzfin"):
            HY[...] = fyz.finish()
            send(HY, HYr, k_fh, dev_xh)
        with stage("fzyfin"):
            fzy.finish(XZ)
            theirs = XZ.at[pl.ds(2 * (1 - xl), 2)]
            send(theirs, XZr.at[0], k_xz, dev_x)
            send(theirs, XZr.at[1], k_xz, dev_x2)
            send(XZ.at[pl.ds(2 * xl, 2)], XZr.at[2], k_xz, dev_xh)
        with stage("fhfin"):
            arrived(HYr, k_fh)
            FY[:, z] = add(HY[...], HYr[...])
            fay[0].start()
            fay[1].start()
        with stage("fxm"):
            arrived(XZr, k_xz)
            near = XZr[0].astype(F32) + XZr[1].astype(F32)
            FZ[:, z] = ((XZ[pl.ds(2 * xl, 2)].astype(F32) + XZr[2].astype(F32)) + near).astype(BF16)
            faz[0].start()
            faz[1].start()
        with stage("fayrelay"):
            fay[0].relay()
            fay[1].relay()
        with stage("fazrelay"):
            faz[0].relay()
            faz[1].relay()
        with stage("fafin"):
            fay[0].finish()
            send(FY.at[0], FY.at[0], k_fpy, core)
            faz[0].finish()
            send(FZ.at[0], FZ.at[0], k_fpz, core)
            fay[1].finish()
            faz[1].finish()

    @pl.when(c == 0)
    def _():
        kept, groups[:] = list(groups), []
        with stage("waitB"):
            loaded(2)
        for t in range(4):
            with stage("grad"):
                both(gradient, t)
                d = order[t]
                for h, to in halves(XB * T):
                    send(WX.at[1 - xl, d, h, :], RX.at[d, h, :], k_gx[t], to)
                leave(gy, t)
        for t in range(4):
            with stage("gx"):
                d = order[t]
                arrived(RX.at[d], k_gx[t])
                VX[d, 0] = add(WX[xl, d], RX[d])
                leave(gxy, t)
            if t == 1:
                with stage("gymid"):
                    gy.middle()
            if t == 2:
                with stage("gxymid"):
                    gxy.middle()
        with stage("gyfin"):
            gy.finish(XG)
            for h, to in halves(HB * T):
                send(XG.at[1 - xl, h, :], XGr.at[h, :], k_xg, to)
        with stage("gxyfin"):
            gxy.finish(YX)
            pieces(UG, 0, HB, YX[0], XB)
        with stage("gxfin"):
            arrived(XGr, k_xg)
            pieces(UG, 0, 0, add(XG[xl], XGr[...]), HB)
            gz.start()
        with stage("gzmid"):
            gz.middle()
        with stage("gzfin"):
            HG[...] = gz.finish()[0]
            send(HG, HGr, k_gh, dev_xh)
        with stage("ghfin"):
            arrived(HGr, k_gh)
            GA[z] = add(HG[...], HGr[...])
            ga.start()
        with stage("waitF"):
            arrived(FY.at[0], k_fpy)
            arrived(FZ.at[0], k_fpz)
        groupsG.extend(groups)
        groups[:] = kept

    with stage("damp"):
        for k, (p, q) in enumerate(UPPER):
            if k < ZF:
                block = FZ[c, :, 16 * k : 16 * (k + 1), :]
            else:
                block = FY[c, :, 16 * (k - ZF) : 16 * (k - ZF + 1), :]
            block = block.reshape(T, T).astype(F32)
            Fm[p * T : (p + 1) * T, q * T : (q + 1) * T] = block
            if p != q:
                Fm[q * T : (q + 1) * T, p * T : (p + 1) * T] = block.T
        eye = (
            lax.broadcasted_iota(jnp.int32, (D, D), 0) == lax.broadcasted_iota(jnp.int32, (D, D), 1)
        ).astype(F32)
        f = Fm[...]
        trace = jnp.sum(jnp.sum(f * eye, axis=0, keepdims=True), axis=1, keepdims=True)
        damped = f + (trace * (0.05 / D)) * eye
        square = jnp.sum(jnp.sum(damped * damped, axis=0, keepdims=True), axis=1, keepdims=True)
        inverse_size = 1.0 / jnp.sqrt(square + 1e-06)
        Pm[...] = eye - damped * inverse_size

    with stage("ns1"):
        r = split(Pm[...])
        Fm[...] = dot3(r, r)
    @pl.when(c == 0)
    def _():
        kept, groups[:] = list(groups), groupsG
        with stage("garelay"):
            ga.relay()
        groupsG[:], groups[:] = list(groups), kept

    with stage("ns2"):
        r1 = split(Fm[...])
        Qm[...] = dot3(r1, r1)

    with stage("ns3"):
        Pm[...] = eye + Pm[...] + Fm[...] + dot3(r, r1)

    with stage("ns4"):
        r2 = split(Qm[...])
        Fm[...] = dot3(r2, r2)
        Pm[...] = Pm[...] + dot3(split(Pm[...]), r2)

    @pl.when(c == 0)
    def _():
        with stage("gafin"):
            ga.finish()
            remote(GA, GA, k_gp, core, LAST + 5).start()

    with stage("ns5"):
        r3 = split(Fm[...])
        X[0], X[1] = split((Pm[...] + dot3(split(Pm[...]), r3)) * inverse_size)

    lo, hi = pl.ds(0, R), pl.ds(R, R)
    out_lo, out_hi = out.at[0, lo, :], out.at[0, hi, :]

    def gather():
        for k in range(GB):
            p, q = k // 4, k % 4
            Gm[p * T : (p + 1) * T, q * T : (q + 1) * T] = GA[:, 16 * k : 16 * (k + 1), :].reshape(T, T)

    @pl.when(c == 1)
    def _():
        remote(X, Xp, k_x, core, LAST + 3).start()
        with stage("waitG"):
            arrived(GA, k_gp)
        with stage("gather"):
            gather()
            right = split(dot(Gm[...], X[0]) + dot(Gm[...], X[1]))
        with stage("waitX"):
            arrived(Xp.at[:, hi, :], k_x)
        with stage("last"):
            mine[...] = dot3((Xp[0, hi, :], Xp[1, hi, :]), right).astype(BF16)
            remote(mine, out_hi, k_out, core, LAST + 4).start()
            pltpu.make_async_copy(mine, out_hi, local_sem.at[3]).start()
        with stage("drain"):
            remote(X, Xp, k_x, core, LAST + 3).wait_send()
            sent(groups)

    @pl.when(c == 0)
    def _():
        theirs = X.at[:, hi, :], Xp.at[:, hi, :]
        remote(*theirs, k_x, core, LAST + 3).start()
        with stage("gather"):
            gather()
            left = split(dot(X[0, lo, :], Gm[...]) + dot(X[1, lo, :], Gm[...]))
        with stage("waitX"):
            arrived(Xp, k_x)
        with stage("last"):
            mine[...] = dot3(left, (Xp[0], Xp[1])).astype(BF16)
            remote(mine, out_lo, k_out, core, LAST + 4).start()
            pltpu.make_async_copy(mine, out_lo, local_sem.at[3]).start()
        with stage("drain"):
            remote(*theirs, k_x, core, LAST + 3).wait_send()
            remote(GA, GA, k_gp, core, LAST + 5).wait_send()
            sent(groupsG)

    with stage("waitO"):
        pltpu.make_async_copy(mine, out_lo, local_sem.at[3]).wait()
        arrived(out_lo, k_out)
        remote(mine, out_lo, k_out, core, LAST + 4).wait_send()
        for src, dst, k, g in gets:
            remote(src, dst, k, core, g).wait_send()
    assert used[0] == NSEM, used[0]


FENCE = True
LAG = 3
AT_FX = (9, 12)
SENT = 2 * 1024 * 1024
NSEM = 79
LAST = 6
NSEND = LAST + 6


def local_step(edge_in, edge_grad, row_mask, layer_at):
    def v(*shape, dtype=BF16):
        return pltpu.VMEM(shape, dtype)

    def ystage(m, rows):
        return [v(4, m, rows, T), v(2, m, rows // 2, T), v(2, 2, m, rows // 2, T)]

    def zpair(m, rows):
        return [v(NZ, 1, m, rows, T), v(3, m, rows, T), v(4, m, rows, T)]

    def zring(chunks, m, rows):
        return [v(NZ, chunks, m, rows, T), v(4, chunks, 2, m, rows, T)]

    yf, hb, xb = YF * T, HB * T, XB * T
    any_ = pl.BlockSpec(memory_space=pl.ANY)
    return pl.pallas_call(
        kernel,
        out_shape=jax.ShapeDtypeStruct((1, D, D), BF16),
        in_specs=[pl.BlockSpec(memory_space=pltpu.SMEM), any_, any_, any_],
        out_specs=any_,
        scratch_shapes=[
            v(L, 2 * R, dtype=jnp.int32), v(L, 2 * R, D), v(L, 2 * R, D), v(SENT // (2 * D), D),
            *zring(8, 2, ZP), *ystage(4, ZP), v(4, ZP, T), v(3, 2, ZP, T),
            *ystage(2, yf), *ystage(2, yf), v(2, 2, yf, T), v(2, yf, T), *zpair(2, YP), v(2, YP, T), v(2, YP, T),
            v(2, NZ, ZP, T), v(2, NZ, YP, T),
            *ystage(2, hb), v(2, hb, T), v(hb, T), v(2, 4, xb, T), v(4, xb, T), *ystage(1, xb), v(1, xb, T),
            *zpair(1, GP), v(GP, T), v(GP, T), v(NZ, GP, T),
            v(D, D, dtype=F32), v(D, D, dtype=F32), v(D, D, dtype=F32), v(D, D), v(2, D, D), v(2, D, D), v(R, D),
            pltpu.SemaphoreType.DMA((4,)), pltpu.SemaphoreType.DMA((NSEND,)), pltpu.SemaphoreType.DMA((NSEM,)),
        ],
        compiler_params=pltpu.CompilerParams(
            collective_id=0, has_side_effects=True, vmem_limit_bytes=60 * 1024 * 1024
        ),
    )(layer_at, row_mask, edge_in, edge_grad)


def solution(mesh):
    rows = P(None, ("dp", "owner"), None)
    return jax.shard_map(
        local_step, mesh=mesh, in_specs=(rows, rows, P(None, ("dp", "owner")), P()),
        out_specs=P("owner", None, None), check_vma=False,
    )
```

```python
import contextlib
import math

import jax
import jax.numpy as jnp
from jax import lax
from jax.experimental import pallas as pl
from jax.experimental.pallas import tpu as pltpu
from jax.sharding import PartitionSpec as P

MESH = pl.DeviceIdType.MESH
F32 = jnp.float32
BF16 = jnp.bfloat16
L = 8
D = 512
R = 256
NZ = 8
T = 128
UPPER = [(i, j) for i in range(4) for j in range(i, 4)]
NF = len(UPPER)
ZF = 7
YF = NF - ZF
ZP, YP = 16 * ZF, 16 * YF
GB = 16
HB = 4
XB = GB - HB
GP = 16 * GB


def add(a, b):
    return (a.astype(F32) + b.astype(F32)).astype(BF16)


def split(x):
    hi = x.astype(BF16)
    return hi, (x - hi.astype(F32)).astype(BF16)


def dot(a, b):
    return lax.dot_general(a, b, (((1,), (0,)), ((), ())), preferred_element_type=F32)


def dot3(a, b):
    (ah, al), (bh, bl) = a, b
    return dot(ah, bh) + (dot(ah, bl) + dot(al, bh))


def kernel(
    layer_at, mask_hbm, in_hbm, grad_hbm, out,
    mask, rows_in, rows_grad, dummy,
    WZ, RZ, VZ, RZr, RZd, XZ, XZr,
    WY0, RY0r, RY0d, WY1, RY1r, RY1d, XY, XYr, UY, RUr, RUd, HY, HYr, FZ, FY,
    WG, RGr, RGd, XG, XGr, WX, RX, VX, RXr, RXd, YX, UG, RUGr, RUGd, HG, HGr, GA,
    Fm, Pm, Qm, Gm, X, Xp, mine, local_sem, send_sem, recv_sem,
):
    dp, ow = lax.axis_index("dp"), lax.axis_index("owner")
    z, xh, c = dp // 4, (dp // 2) % 2, dp % 2
    xl, y = ow // 4, ow % 4

    def dev(z=z, xh=xh, c=c, xl=xl, y=y):
        return (z * 4 + xh * 2 + c, xl * 4 + y)

    ya = y + 1 - 2 * (y % 2)
    yb = 3 - y
    yo = (y + 2) % 4
    core = dev(c=1 - c)
    dev_ya, dev_yb = dev(y=ya), dev(y=yb)
    dev_x, dev_x2, dev_xh = dev(xl=1 - xl), dev(xl=1 - xl, xh=1 - xh), dev(xh=1 - xh)
    up, down = dev(z=(z + 1) % NZ), dev(z=(z + NZ - 1) % NZ)

    used = [0]
    groups, groupsG = [], []

    def ids():
        used[0] += 1
        return used[0] - 1

    def remote(src, dst, k, to, g=0):
        return pltpu.make_async_remote_copy(
            src_ref=src, dst_ref=dst, send_sem=send_sem.at[g], recv_sem=recv_sem.at[k],
            device_id=to, device_id_type=MESH,
        )

    def send(src, dst, k, to):
        size = math.prod(src.shape) * src.dtype.itemsize
        if not groups or groups[-1] + size > SENT:
            groups.append(0)
        groups[-1] += size
        remote(src, dst, k, to, len(groups) - 1).start()

    def sent(groups):
        for g, size in enumerate(groups):
            ref = dummy.at[pl.ds(0, size // (2 * D))]
            pltpu.make_async_copy(ref, ref, send_sem.at[g]).wait()
        assert len(groups) <= LAST, len(groups)

    def arrived(dst, k):
        remote(dst, dst, k, core).wait_recv()

    @contextlib.contextmanager
    def stage(name):
        with jax.named_scope(name):
            yield
        if FENCE:
            pl.delay(1)

    barrier = pltpu.get_barrier_semaphore()
    up2, down2 = dev(z=(z + 2) % NZ), dev(z=(z + NZ - 2) % NZ)
    peers = (core, dev_ya, dev_yb, dev_x, dev_x2, dev_xh, up, down, up2, down2)
    for peer in peers:
        pl.semaphore_signal(barrier, inc=1, device_id=peer, device_id_type=MESH)

    own, other = pl.ds(0, R), pl.ds(R, R)
    loads = ((mask_hbm, mask.at[:, own]), (in_hbm, rows_in.at[:, own, :]), (grad_hbm, rows_grad.at[:, own, :]))
    gets = [(mask_hbm, mask.at[:, other]), (in_hbm, rows_in.at[:, other, :]), (grad_hbm, rows_grad.at[:, other, :])]
    gets = [(src, dst, ids(), LAST + i) for i, (src, dst) in enumerate(gets)]
    for i, (src, dst) in enumerate(loads):
        pltpu.make_async_copy(src, dst, local_sem.at[i]).start()
    with stage("barrier"):
        pl.semaphore_wait(barrier, len(peers))
        for src, dst, k, g in gets:
            remote(src, dst, k, core, g).start()

    def loaded(i):
        src, dst = loads[i]
        pltpu.make_async_copy(src, dst, local_sem.at[i]).wait()
        arrived(gets[i][1], gets[i][2])

    with stage("waitA"):
        loaded(0)
        loaded(1)

    dirs = ((1, up, up2), (-1, down, down2))

    def zd(direction, far):
        return (z + NZ + direction * far) % NZ

    class ZRing:
        def __init__(self, W, Rz, rows, chunks):
            self.W, self.Rz = W, Rz
            self.k = [[ids() for _ in range(chunks)] for _ in range(4)]
            self.half = [pl.ds(0, rows // 2), pl.ds(rows // 2, rows // 2)]

        def go(self, n, s, q, half=None):
            w, r = self.W.at[zd(dirs[n][0], 4 - s), q], self.Rz.at[s, q, n]
            if half is not None:
                w, r = w.at[:, half, :], r.at[:, half, :]
            send(w, r, self.k[s][q], dirs[n][1])

        def start(self, q=0):
            for n in range(2):
                self.go(n, 0, q, self.half[n])
            for n in range(2):
                self.go(n, 1, q, self.half[1 - n])

        def step(self, s, q=0):
            arrived(self.Rz.at[s - 1, q, 0] if s == 1 else self.Rz.at[s - 1, q], self.k[s - 1][q])
            for n in range(2):
                d = zd(dirs[n][0], 4 - s)
                if s == 1:
                    h = self.half[n]
                    self.W[d, q, :, h, :] = add(self.W[d, q, :, h, :], self.Rz[0, q, n, :, h, :])
                    self.go(n, 1, q, h)
                else:
                    self.W[d, q] = add(self.W[d, q], self.Rz[s - 1, q, n])
                    self.go(n, s, q)

        def finish(self, q=0):
            arrived(self.Rz.at[3, q], self.k[3][q])
            mine = self.W[z, q].astype(F32)
            return (mine + (self.Rz[3, q, 0].astype(F32) + self.Rz[3, q, 1].astype(F32))).astype(BF16)

    class YStage:
        def __init__(self, W, Rr, Rd, rows):
            self.W, self.Rr, self.Rd = W, Rr, Rd
            self.kr, self.kd = ids(), ids()
            h = rows // 2
            self.half = [pl.ds(0, h), pl.ds(h, h)]

        def relay(self):
            for s, to in enumerate((dev_ya, dev_yb)):
                send(self.W.at[yo, :, self.half[s], :], self.Rr.at[s], self.kr, to)

        def direct(self, s):
            d, to = ((ya, dev_ya), (yb, dev_yb))[s]
            send(self.W.at[d, :, self.half[s], :], self.Rd.at[0, s], self.kd, to)

        def start(self):
            self.relay()
            self.direct(0)
            self.direct(1)

        def middle(self):
            arrived(self.Rr, self.kr)
            for s, (d, to) in enumerate(((yb, dev_yb), (ya, dev_ya))):
                h = self.half[s]
                self.W[d, :, h, :] = add(self.W[d, :, h, :], self.Rr[s])
                send(self.W.at[d, :, h, :], self.Rd.at[1, s], self.kd, to)

        def finish(self, out):
            arrived(self.Rd, self.kd)
            for s in range(2):
                h = self.half[s]
                total = self.W[y, :, h, :].astype(F32) + (self.Rd[0, s].astype(F32) + self.Rd[1, s].astype(F32))
                out[:, h, :] = total.astype(BF16)

    class ZPair:
        def __init__(self, W, Rr, Rd, rows):
            self.W, self.Rr, self.Rd, self.kr, self.kd = W, Rr, Rd, ids(), ids()
            self.half = [pl.ds(0, rows // 2), pl.ds(rows // 2, rows // 2)]

        def start(self):
            W, Rr = self.W, self.Rr
            for n, (direction, to, to2) in enumerate(dirs):
                h = self.half[n]
                send(W.at[zd(direction, 4), 0, :, h, :], Rr.at[2, :, h, :], self.kr, to2)
                send(W.at[zd(direction, 3), 0], Rr.at[n], self.kr, to)
            for n, (direction, to, to2) in enumerate(dirs):
                send(W.at[zd(direction, 1), 0], self.Rd.at[n], self.kd, to)

        def middle(self):
            W, Rr = self.W, self.Rr
            arrived(Rr, self.kr)
            for n, (direction, to, to2) in enumerate(dirs):
                d = zd(direction, 2)
                near, far = self.half[1 - n], self.half[n]
                W[d, 0, :, near, :] = add(W[d, 0, :, near, :], Rr[n, :, near, :])
                both = Rr[n, :, far, :].astype(F32) + Rr[2, :, far, :].astype(F32)
                W[d, 0, :, far, :] = (W[d, 0, :, far, :].astype(F32) + both).astype(BF16)
                send(W.at[d, 0], self.Rd.at[2 + n], self.kd, to2)

        def finish(self):
            Rd = self.Rd
            arrived(Rd, self.kd)
            near = Rd[0].astype(F32) + Rd[1].astype(F32)
            far = Rd[2].astype(F32) + Rd[3].astype(F32)
            return ((self.W[z, 0].astype(F32) + near) + far).astype(BF16)

    class AllGather:
        def __init__(self, A, rows):
            self.A, self.k = A, [ids() for _ in range(3)]
            self.half = [pl.ds(0, rows // 2), pl.ds(rows // 2, rows // 2)]

        def start(self):
            p = self.A.at[z]
            for direction, to, to2 in dirs:
                send(p, p, self.k[1], to2)
            for direction, to, to2 in dirs:
                send(p, p, self.k[0], to)

        def relay(self):
            arrived(self.A.at[pl.ds(0, 2)], self.k[1])
            for n, (direction, to, to2) in enumerate(dirs):
                p = self.A.at[zd(-direction, 2), self.half[n], :]
                send(p, p, self.k[2], to2)
            for n, (direction, to, to2) in enumerate(dirs):
                p = self.A.at[zd(-direction, 2)]
                send(p, p, self.k[2], to)

        def finish(self):
            arrived(self.A.at[pl.ds(0, 2)], self.k[0])
            arrived(self.A.at[pl.ds(0, 3)], self.k[2])

    order = (yo, ya, yb, y)
    fz = ZRing(WZ, RZ, ZP, 8)
    fzy = YStage(VZ, RZr, RZd, ZP)
    fy = (YStage(WY0, RY0r, RY0d, YF * T), YStage(WY1, RY1r, RY1d, YF * T))
    fyz = ZPair(UY, RUr, RUd, YP)
    faz = (AllGather(FZ.at[0], ZP), AllGather(FZ.at[1], ZP))
    fay = (AllGather(FY.at[0], YP), AllGather(FY.at[1], YP))
    gy = YStage(WG, RGr, RGd, HB * T)
    gxy = YStage(VX, RXr, RXd, XB * T)
    gz = ZPair(UG, RUGr, RUGd, GP)
    ga = AllGather(GA, GP)
    k_fx = [ids() for _ in range(2)]
    k_gx = [ids() for _ in range(4)]
    k_xz, k_fh, k_gh, k_xg = (ids() for _ in range(4))
    k_fpz, k_fpy, k_gp, k_x, k_out = (ids() for _ in range(5))

    def pieces(ref, m, first, f, n):
        for k in range(n):
            ref[:, 0, m, 16 * (first + k) : 16 * (first + k + 1), :] = f[k * T : (k + 1) * T].reshape(8, 16, T)

    def factor(i, x):
        f, t = i // 4, i % 4
        d = order[t]
        layer = layer_at[x * 4 + d]
        a = (rows_in, rows_grad)[f][layer]
        m = mask[pl.ds(layer, 1), :].astype(F32).astype(BF16)
        am = a.T * m
        top = dot(am[:R], a) * (1.0 / 65536)
        low = dot(am[R:], a[:, R:]) * (1.0 / 65536)
        for k, (p, q) in enumerate(UPPER):
            if p < 2:
                block = top[p * T : (p + 1) * T, q * T : (q + 1) * T].astype(BF16)
            else:
                block = low[(p - 2) * T : (p - 1) * T, (q - 2) * T : (q - 1) * T].astype(BF16)
            if k < ZF:
                WZ[:, i, x, 16 * k : 16 * (k + 1), :] = block.reshape(8, 16, T)
            else:
                (WY0, WY1)[f][d, x, (k - ZF) * T : (k - ZF + 1) * T, :] = block

    def gradient(t, x):
        d = order[t]
        layer = layer_at[x * 4 + d]
        g = (dot(rows_in[layer].T, rows_grad[layer]) * (1.0 / 256)).astype(BF16)
        for k in range(GB):
            p, q = k // 4, k % 4
            block = g[p * T : (p + 1) * T, q * T : (q + 1) * T]
            if k < HB:
                WG[d, x, k * T : (k + 1) * T, :] = block
            else:
                WX[x, d, (k - HB) * T : (k - HB + 1) * T, :] = block

    def both(f, t):
        lax.fori_loop(0, 2, lambda x, carry: (f(t, x), carry)[1], 0)

    def leave(ystage, t):
        if t == 0:
            ystage.relay()
        elif t < 3:
            ystage.direct(t - 1)

    def halves(rows):
        return (pl.ds(0, rows // 2), dev_x), (pl.ds(rows // 2, rows // 2), dev_x2)


    @pl.when(c == 1)
    def _():
        def fx(f):
            with stage("fyfin"):
                fy[f].finish(XY.at[f])
                for h, to in halves(YF * T):
                    send(XY.at[f, 1 - xl, h, :], XYr.at[f, h, :], k_fx[f], to)

        for i in range(8 + 3 * LAG):
            if i < 8:
                f, t = i // 4, i % 4
                with stage(f"factor{i}"):
                    if i == 4:
                        loaded(2)
                    both(factor, i)
                    fz.start(i)
                    leave(fy[f], t)
            for s in (3, 2, 1):
                if 0 <= i - s * LAG < 8:
                    with stage(f"fz{s}"):
                        fz.step(s, i - s * LAG)
            if i == 4:
                with stage("fy0mid"):
                    fy[0].middle()
            if i == 8:
                with stage("fy1mid"):
                    fy[1].middle()
            if i in AT_FX:
                fx(AT_FX.index(i))
        with stage("fxfin"):
            for f in range(2):
                arrived(XYr.at[f], k_fx[f])
                pieces(UY, f, 0, add(XY[f, xl], XYr[f]), YF)
            fyz.start()
        for t in range(4):
            with stage("fzfin"):
                for f in range(2):
                    v = fz.finish(4 * f + t)
                    for x in range(2):
                        VZ[order[t], 2 * x + f] = v[x]
                leave(fzy, t)
        with stage("fyzmid"):
            fyz.middle()
        with stage("fzymid"):
            fzy.middle()
        with stage("fyzfin"):
            HY[...] = fyz.finish()
            send(HY, HYr, k_fh, dev_xh)
        with stage("fzyfin"):
            fzy.finish(XZ)
            theirs = XZ.at[pl.ds(2 * (1 - xl), 2)]
            send(theirs, XZr.at[0], k_xz, dev_x)
            send(theirs, XZr.at[1], k_xz, dev_x2)
            send(XZ.at[pl.ds(2 * xl, 2)], XZr.at[2], k_xz, dev_xh)
        with stage("fhfin"):
            arrived(HYr, k_fh)
            FY[:, z] = add(HY[...], HYr[...])
            fay[0].start()
            fay[1].start()
        with stage("fxm"):
            arrived(XZr, k_xz)
            near = XZr[0].astype(F32) + XZr[1].astype(F32)
            FZ[:, z] = ((XZ[pl.ds(2 * xl, 2)].astype(F32) + XZr[2].astype(F32)) + near).astype(BF16)
            faz[0].start()
            faz[1].start()
        with stage("fayrelay"):
            fay[0].relay()
            fay[1].relay()
        with stage("fazrelay"):
            faz[0].relay()
            faz[1].relay()
        with stage("fafin"):
            fay[0].finish()
            send(FY.at[0], FY.at[0], k_fpy, core)
            faz[0].finish()
            send(FZ.at[0], FZ.at[0], k_fpz, core)
            fay[1].finish()
            faz[1].finish()

    @pl.when(c == 0)
    def _():
        kept, groups[:] = list(groups), []
        with stage("waitB"):
            loaded(2)
        for t in range(4):
            with stage("grad"):
                both(gradient, t)
                d = order[t]
                for h, to in halves(XB * T):
                    send(WX.at[1 - xl, d, h, :], RX.at[d, h, :], k_gx[t], to)
                leave(gy, t)
        for t in range(4):
            with stage("gx"):
                d = order[t]
                arrived(RX.at[d], k_gx[t])
                VX[d, 0] = add(WX[xl, d], RX[d])
                leave(gxy, t)
            if t == 1:
                with stage("gymid"):
                    gy.middle()
            if t == 2:
                with stage("gxymid"):
                    gxy.middle()
        with stage("gyfin"):
            gy.finish(XG)
            for h, to in halves(HB * T):
                send(XG.at[1 - xl, h, :], XGr.at[h, :], k_xg, to)
        with stage("gxyfin"):
            gxy.finish(YX)
            pieces(UG, 0, HB, YX[0], XB)
        with stage("gxfin"):
            arrived(XGr, k_xg)
            pieces(UG, 0, 0, add(XG[xl], XGr[...]), HB)
            gz.start()
        with stage("gzmid"):
            gz.middle()
        with stage("gzfin"):
            HG[...] = gz.finish()[0]
            send(HG, HGr, k_gh, dev_xh)
        with stage("ghfin"):
            arrived(HGr, k_gh)
            GA[z] = add(HG[...], HGr[...])
            ga.start()
        with stage("waitF"):
            arrived(FY.at[0], k_fpy)
            arrived(FZ.at[0], k_fpz)
        groupsG.extend(groups)
        groups[:] = kept

    with stage("damp"):
        for k, (p, q) in enumerate(UPPER):
            if k < ZF:
                block = FZ[c, :, 16 * k : 16 * (k + 1), :]
            else:
                block = FY[c, :, 16 * (k - ZF) : 16 * (k - ZF + 1), :]
            block = block.reshape(T, T).astype(F32)
            Fm[p * T : (p + 1) * T, q * T : (q + 1) * T] = block
            if p != q:
                Fm[q * T : (q + 1) * T, p * T : (p + 1) * T] = block.T
        eye = (
            lax.broadcasted_iota(jnp.int32, (D, D), 0) == lax.broadcasted_iota(jnp.int32, (D, D), 1)
        ).astype(F32)
        f = Fm[...]
        trace = jnp.sum(jnp.sum(f * eye, axis=0, keepdims=True), axis=1, keepdims=True)
        damped = f + (trace * (0.05 / D)) * eye
        square = jnp.sum(jnp.sum(damped * damped, axis=0, keepdims=True), axis=1, keepdims=True)
        inverse_size = 1.0 / jnp.sqrt(square + 1e-06)
        Pm[...] = eye - damped * inverse_size

    with stage("ns1"):
        r = split(Pm[...])
        Fm[...] = dot3(r, r)
    @pl.when(c == 0)
    def _():
        kept, groups[:] = list(groups), groupsG
        with stage("garelay"):
            ga.relay()
        groupsG[:], groups[:] = list(groups), kept

    with stage("ns2"):
        r1 = split(Fm[...])
        Qm[...] = dot3(r1, r1)

    with stage("ns3"):
        Pm[...] = eye + Pm[...] + Fm[...] + dot3(r, r1)

    with stage("ns4"):
        r2 = split(Qm[...])
        Fm[...] = dot3(r2, r2)
        Pm[...] = Pm[...] + dot3(split(Pm[...]), r2)

    @pl.when(c == 0)
    def _():
        with stage("gafin"):
            ga.finish()
            remote(GA, GA, k_gp, core, LAST + 5).start()

    with stage("ns5"):
        r3 = split(Fm[...])
        X[0], X[1] = split((Pm[...] + dot3(split(Pm[...]), r3)) * inverse_size)

    lo, hi = pl.ds(0, R), pl.ds(R, R)
    out_lo, out_hi = out.at[0, lo, :], out.at[0, hi, :]

    def gather():
        for k in range(GB):
            p, q = k // 4, k % 4
            Gm[p * T : (p + 1) * T, q * T : (q + 1) * T] = GA[:, 16 * k : 16 * (k + 1), :].reshape(T, T)

    @pl.when(c == 1)
    def _():
        remote(X, Xp, k_x, core, LAST + 3).start()
        with stage("waitG"):
            arrived(GA, k_gp)
        with stage("gather"):
            gather()
            right = split(dot(Gm[...], X[0]) + dot(Gm[...], X[1]))
        with stage("waitX"):
            arrived(Xp.at[:, hi, :], k_x)
        with stage("last"):
            mine[...] = dot3((Xp[0, hi, :], Xp[1, hi, :]), right).astype(BF16)
            remote(mine, out_hi, k_out, core, LAST + 4).start()
            pltpu.make_async_copy(mine, out_hi, local_sem.at[3]).start()
        with stage("drain"):
            remote(X, Xp, k_x, core, LAST + 3).wait_send()
            sent(groups)

    @pl.when(c == 0)
    def _():
        theirs = X.at[:, hi, :], Xp.at[:, hi, :]
        remote(*theirs, k_x, core, LAST + 3).start()
        with stage("gather"):
            gather()
            left = split(dot(X[0, lo, :], Gm[...]) + dot(X[1, lo, :], Gm[...]))
        with stage("waitX"):
            arrived(Xp, k_x)
        with stage("last"):
            mine[...] = dot3(left, (Xp[0], Xp[1])).astype(BF16)
            remote(mine, out_lo, k_out, core, LAST + 4).start()
            pltpu.make_async_copy(mine, out_lo, local_sem.at[3]).start()
        with stage("drain"):
            remote(*theirs, k_x, core, LAST + 3).wait_send()
            remote(GA, GA, k_gp, core, LAST + 5).wait_send()
            sent(groupsG)

    with stage("waitO"):
        pltpu.make_async_copy(mine, out_lo, local_sem.at[3]).wait()
        arrived(out_lo, k_out)
        remote(mine, out_lo, k_out, core, LAST + 4).wait_send()
        for src, dst, k, g in gets:
            remote(src, dst, k, core, g).wait_send()
    assert used[0] == NSEM, used[0]


FENCE = True
LAG = 3
AT_FX = (9, 12)
SENT = 2 * 1024 * 1024
NSEM = 79
LAST = 6
NSEND = LAST + 6


def local_step(edge_in, edge_grad, row_mask, layer_at):
    def v(*shape, dtype=BF16):
        return pltpu.VMEM(shape, dtype)

    def ystage(m, rows):
        return [v(4, m, rows, T), v(2, m, rows // 2, T), v(2, 2, m, rows // 2, T)]

    def zpair(m, rows):
        return [v(NZ, 1, m, rows, T), v(3, m, rows, T), v(4, m, rows, T)]

    def zring(chunks, m, rows):
        return [v(NZ, chunks, m, rows, T), v(4, chunks, 2, m, rows, T)]

    yf, hb, xb = YF * T, HB * T, XB * T
    any_ = pl.BlockSpec(memory_space=pl.ANY)
    return pl.pallas_call(
        kernel,
        out_shape=jax.ShapeDtypeStruct((1, D, D), BF16),
        in_specs=[pl.BlockSpec(memory_space=pltpu.SMEM), any_, any_, any_],
        out_specs=any_,
        scratch_shapes=[
            v(L, 2 * R, dtype=jnp.int32), v(L, 2 * R, D), v(L, 2 * R, D), v(SENT // (2 * D), D),
            *zring(8, 2, ZP), *ystage(4, ZP), v(4, ZP, T), v(3, 2, ZP, T),
            *ystage(2, yf), *ystage(2, yf), v(2, 2, yf, T), v(2, yf, T), *zpair(2, YP), v(2, YP, T), v(2, YP, T),
            v(2, NZ, ZP, T), v(2, NZ, YP, T),
            *ystage(2, hb), v(2, hb, T), v(hb, T), v(2, 4, xb, T), v(4, xb, T), *ystage(1, xb), v(1, xb, T),
            *zpair(1, GP), v(GP, T), v(GP, T), v(NZ, GP, T),
            v(D, D, dtype=F32), v(D, D, dtype=F32), v(D, D, dtype=F32), v(D, D), v(2, D, D), v(2, D, D), v(R, D),
            pltpu.SemaphoreType.DMA((4,)), pltpu.SemaphoreType.DMA((NSEND,)), pltpu.SemaphoreType.DMA((NSEM,)),
        ],
        compiler_params=pltpu.CompilerParams(
            collective_id=0, has_side_effects=True, vmem_limit_bytes=60 * 1024 * 1024
        ),
    )(layer_at, row_mask, edge_in, edge_grad)


def solution(mesh):
    rows = P(None, ("dp", "owner"), None)
    return jax.shard_map(
        local_step, mesh=mesh, in_specs=(rows, rows, P(None, ("dp", "owner")), P()),
        out_specs=P("owner", None, None), check_vma=False,
    )
```

```python
import contextlib
import math

import jax
import jax.numpy as jnp
from jax import lax
from jax.experimental import pallas as pl
from jax.experimental.pallas import tpu as pltpu
from jax.sharding import PartitionSpec as P

MESH = pl.DeviceIdType.MESH
F32 = jnp.float32
BF16 = jnp.bfloat16
L = 8
D = 512
R = 256
NZ = 8
T = 128
UPPER = [(i, j) for i in range(4) for j in range(i, 4)]
NF = len(UPPER)
ZF = 7
YF = NF - ZF
ZP, YP = 16 * ZF, 16 * YF
GB = 16
HB = 4
XB = GB - HB
GP = 16 * GB


def add(a, b):
    return (a.astype(F32) + b.astype(F32)).astype(BF16)


def split(x):
    hi = x.astype(BF16)
    return hi, (x - hi.astype(F32)).astype(BF16)


def dot(a, b):
    return lax.dot_general(a, b, (((1,), (0,)), ((), ())), preferred_element_type=F32)


def dot3(a, b):
    (ah, al), (bh, bl) = a, b
    return dot(ah, bh) + (dot(ah, bl) + dot(al, bh))


def kernel(
    layer_at, mask_hbm, in_hbm, grad_hbm, out,
    mask, rows_in, rows_grad, dummy,
    WZ, RZ, VZ, RZr, RZd, XZ, XZr,
    WY0, RY0r, RY0d, WY1, RY1r, RY1d, XY, XYr, UY, RUr, RUd, HY, HYr, FZ, FY,
    WG, RGr, RGd, XG, XGr, WX, RX, VX, RXr, RXd, YX, UG, RUGr, RUGd, HG, HGr, GA,
    Fm, Pm, Qm, Gm, X, Xp, mine, local_sem, send_sem, recv_sem,
):
    dp, ow = lax.axis_index("dp"), lax.axis_index("owner")
    z, xh, c = dp // 4, (dp // 2) % 2, dp % 2
    xl, y = ow // 4, ow % 4

    def dev(z=z, xh=xh, c=c, xl=xl, y=y):
        return (z * 4 + xh * 2 + c, xl * 4 + y)

    ya = y + 1 - 2 * (y % 2)
    yb = 3 - y
    yo = (y + 2) % 4
    core = dev(c=1 - c)
    dev_ya, dev_yb = dev(y=ya), dev(y=yb)
    dev_x, dev_x2, dev_xh = dev(xl=1 - xl), dev(xl=1 - xl, xh=1 - xh), dev(xh=1 - xh)
    up, down = dev(z=(z + 1) % NZ), dev(z=(z + NZ - 1) % NZ)

    used = [0]
    groups, groupsG = [], []

    def ids():
        used[0] += 1
        return used[0] - 1

    def remote(src, dst, k, to, g=0):
        return pltpu.make_async_remote_copy(
            src_ref=src, dst_ref=dst, send_sem=send_sem.at[g], recv_sem=recv_sem.at[k],
            device_id=to, device_id_type=MESH,
        )

    def send(src, dst, k, to):
        size = math.prod(src.shape) * src.dtype.itemsize
        if not groups or groups[-1] + size > SENT:
            groups.append(0)
        groups[-1] += size
        remote(src, dst, k, to, len(groups) - 1).start()

    def sent(groups):
        for g, size in enumerate(groups):
            ref = dummy.at[pl.ds(0, size // (2 * D))]
            pltpu.make_async_copy(ref, ref, send_sem.at[g]).wait()
        assert len(groups) <= LAST, len(groups)

    def arrived(dst, k):
        remote(dst, dst, k, core).wait_recv()

    @contextlib.contextmanager
    def stage(name):
        with jax.named_scope(name):
            yield
        if FENCE:
            pl.delay(1)

    barrier = pltpu.get_barrier_semaphore()
    up2, down2 = dev(z=(z + 2) % NZ), dev(z=(z + NZ - 2) % NZ)
    peers = (core, dev_ya, dev_yb, dev_x, dev_x2, dev_xh, up, down, up2, down2)
    for peer in peers:
        pl.semaphore_signal(barrier, inc=1, device_id=peer, device_id_type=MESH)

    own, other = pl.ds(0, R), pl.ds(R, R)
    loads = ((mask_hbm, mask.at[:, own]), (in_hbm, rows_in.at[:, own, :]), (grad_hbm, rows_grad.at[:, own, :]))
    gets = [(mask_hbm, mask.at[:, other]), (in_hbm, rows_in.at[:, other, :]), (grad_hbm, rows_grad.at[:, other, :])]
    gets = [(src, dst, ids(), LAST + i) for i, (src, dst) in enumerate(gets)]
    for i, (src, dst) in enumerate(loads):
        pltpu.make_async_copy(src, dst, local_sem.at[i]).start()
    with stage("barrier"):
        pl.semaphore_wait(barrier, len(peers))
        for src, dst, k, g in gets:
            remote(src, dst, k, core, g).start()

    def loaded(i):
        src, dst = loads[i]
        pltpu.make_async_copy(src, dst, local_sem.at[i]).wait()
        arrived(gets[i][1], gets[i][2])

    with stage("waitA"):
        loaded(0)
        loaded(1)

    dirs = ((1, up, up2), (-1, down, down2))

    def zd(direction, far):
        return (z + NZ + direction * far) % NZ

    class ZRing:
        def __init__(self, W, Rz, rows, chunks):
            self.W, self.Rz = W, Rz
            self.k = [[ids() for _ in range(chunks)] for _ in range(4)]
            self.half = [pl.ds(0, rows // 2), pl.ds(rows // 2, rows // 2)]

        def go(self, n, s, q, half=None):
            w, r = self.W.at[zd(dirs[n][0], 4 - s), q], self.Rz.at[s, q, n]
            if half is not None:
                w, r = w.at[:, half, :], r.at[:, half, :]
            send(w, r, self.k[s][q], dirs[n][1])

        def start(self, q=0):
            for n in range(2):
                self.go(n, 0, q, self.half[n])
            for n in range(2):
                self.go(n, 1, q, self.half[1 - n])

        def step(self, s, q=0):
            arrived(self.Rz.at[s - 1, q, 0] if s == 1 else self.Rz.at[s - 1, q], self.k[s - 1][q])
            for n in range(2):
                d = zd(dirs[n][0], 4 - s)
                if s == 1:
                    h = self.half[n]
                    self.W[d, q, :, h, :] = add(self.W[d, q, :, h, :], self.Rz[0, q, n, :, h, :])
                    self.go(n, 1, q, h)
                else:
                    self.W[d, q] = add(self.W[d, q], self.Rz[s - 1, q, n])
                    self.go(n, s, q)

        def finish(self, q=0):
            arrived(self.Rz.at[3, q], self.k[3][q])
            mine = self.W[z, q].astype(F32)
            return (mine + (self.Rz[3, q, 0].astype(F32) + self.Rz[3, q, 1].astype(F32))).astype(BF16)

    class YStage:
        def __init__(self, W, Rr, Rd, rows):
            self.W, self.Rr, self.Rd = W, Rr, Rd
            self.kr, self.kd = ids(), ids()
            h = rows // 2
            self.half = [pl.ds(0, h), pl.ds(h, h)]

        def relay(self):
            for s, to in enumerate((dev_ya, dev_yb)):
                send(self.W.at[yo, :, self.half[s], :], self.Rr.at[s], self.kr, to)

        def direct(self, s):
            d, to = ((ya, dev_ya), (yb, dev_yb))[s]
            send(self.W.at[d, :, self.half[s], :], self.Rd.at[0, s], self.kd, to)

        def start(self):
            self.relay()
            self.direct(0)
            self.direct(1)

        def middle(self):
            arrived(self.Rr, self.kr)
            for s, (d, to) in enumerate(((yb, dev_yb), (ya, dev_ya))):
                h = self.half[s]
                self.W[d, :, h, :] = add(self.W[d, :, h, :], self.Rr[s])
                send(self.W.at[d, :, h, :], self.Rd.at[1, s], self.kd, to)

        def finish(self, out):
            arrived(self.Rd, self.kd)
            for s in range(2):
                h = self.half[s]
                total = self.W[y, :, h, :].astype(F32) + (self.Rd[0, s].astype(F32) + self.Rd[1, s].astype(F32))
                out[:, h, :] = total.astype(BF16)

    class ZPair:
        def __init__(self, W, Rr, Rd, rows):
            self.W, self.Rr, self.Rd, self.kr, self.kd = W, Rr, Rd, ids(), ids()
            self.half = [pl.ds(0, rows // 2), pl.ds(rows // 2, rows // 2)]

        def start(self):
            W, Rr = self.W, self.Rr
            for n, (direction, to, to2) in enumerate(dirs):
                h = self.half[n]
                send(W.at[zd(direction, 4), 0, :, h, :], Rr.at[2, :, h, :], self.kr, to2)
                send(W.at[zd(direction, 3), 0], Rr.at[n], self.kr, to)
            for n, (direction, to, to2) in enumerate(dirs):
                send(W.at[zd(direction, 1), 0], self.Rd.at[n], self.kd, to)

        def middle(self):
            W, Rr = self.W, self.Rr
            arrived(Rr, self.kr)
            for n, (direction, to, to2) in enumerate(dirs):
                d = zd(direction, 2)
                near, far = self.half[1 - n], self.half[n]
                W[d, 0, :, near, :] = add(W[d, 0, :, near, :], Rr[n, :, near, :])
                both = Rr[n, :, far, :].astype(F32) + Rr[2, :, far, :].astype(F32)
                W[d, 0, :, far, :] = (W[d, 0, :, far, :].astype(F32) + both).astype(BF16)
                send(W.at[d, 0], self.Rd.at[2 + n], self.kd, to2)

        def finish(self):
            Rd = self.Rd
            arrived(Rd, self.kd)
            near = Rd[0].astype(F32) + Rd[1].astype(F32)
            far = Rd[2].astype(F32) + Rd[3].astype(F32)
            return ((self.W[z, 0].astype(F32) + near) + far).astype(BF16)

    class AllGather:
        def __init__(self, A, rows):
            self.A, self.k = A, [ids() for _ in range(3)]
            self.half = [pl.ds(0, rows // 2), pl.ds(rows // 2, rows // 2)]

        def start(self):
            p = self.A.at[z]
            for direction, to, to2 in dirs:
                send(p, p, self.k[1], to2)
            for direction, to, to2 in dirs:
                send(p, p, self.k[0], to)

        def relay(self):
            arrived(self.A.at[pl.ds(0, 2)], self.k[1])
            for n, (direction, to, to2) in enumerate(dirs):
                p = self.A.at[zd(-direction, 2), self.half[n], :]
                send(p, p, self.k[2], to2)
            for n, (direction, to, to2) in enumerate(dirs):
                p = self.A.at[zd(-direction, 2)]
                send(p, p, self.k[2], to)

        def finish(self):
            arrived(self.A.at[pl.ds(0, 2)], self.k[0])
            arrived(self.A.at[pl.ds(0, 3)], self.k[2])

    order = (yo, ya, yb, y)
    fz = ZRing(WZ, RZ, ZP, 8)
    fzy = YStage(VZ, RZr, RZd, ZP)
    fy = (YStage(WY0, RY0r, RY0d, YF * T), YStage(WY1, RY1r, RY1d, YF * T))
    fyz = ZPair(UY, RUr, RUd, YP)
    faz = (AllGather(FZ.at[0], ZP), AllGather(FZ.at[1], ZP))
    fay = (AllGather(FY.at[0], YP), AllGather(FY.at[1], YP))
    gy = YStage(WG, RGr, RGd, HB * T)
    gxy = YStage(VX, RXr, RXd, XB * T)
    gz = ZPair(UG, RUGr, RUGd, GP)
    ga = AllGather(GA, GP)
    k_fx = [ids() for _ in range(2)]
    k_gx = [ids() for _ in range(4)]
    k_xz, k_fh, k_gh, k_xg = (ids() for _ in range(4))
    k_fpz, k_fpy, k_gp, k_x, k_out = (ids() for _ in range(5))

    def pieces(ref, m, first, f, n):
        for k in range(n):
            ref[:, 0, m, 16 * (first + k) : 16 * (first + k + 1), :] = f[k * T : (k + 1) * T].reshape(8, 16, T)

    def factor(i, x):
        f, t = i // 4, i % 4
        d = order[t]
        layer = layer_at[x * 4 + d]
        a = (rows_in, rows_grad)[f][layer]
        m = mask[pl.ds(layer, 1), :].astype(F32).astype(BF16)
        am = a.T * m
        top = dot(am[:R], a) * (1.0 / 65536)
        low = dot(am[R:], a[:, R:]) * (1.0 / 65536)
        for k, (p, q) in enumerate(UPPER):
            if p < 2:
                block = top[p * T : (p + 1) * T, q * T : (q + 1) * T].astype(BF16)
            else:
                block = low[(p - 2) * T : (p - 1) * T, (q - 2) * T : (q - 1) * T].astype(BF16)
            if k < ZF:
                WZ[:, i, x, 16 * k : 16 * (k + 1), :] = block.reshape(8, 16, T)
            else:
                (WY0, WY1)[f][d, x, (k - ZF) * T : (k - ZF + 1) * T, :] = block

    def gradient(t, x):
        d = order[t]
        layer = layer_at[x * 4 + d]
        g = (dot(rows_in[layer].T, rows_grad[layer]) * (1.0 / 256)).astype(BF16)
        for k in range(GB):
            p, q = k // 4, k % 4
            block = g[p * T : (p + 1) * T, q * T : (q + 1) * T]
            if k < HB:
                WG[d, x, k * T : (k + 1) * T, :] = block
            else:
                WX[x, d, (k - HB) * T : (k - HB + 1) * T, :] = block

    def both(f, t):
        lax.fori_loop(0, 2, lambda x, carry: (f(t, x), carry)[1], 0)

    def leave(ystage, t):
        if t == 0:
            ystage.relay()
        elif t < 3:
            ystage.direct(t - 1)

    def halves(rows):
        return (pl.ds(0, rows // 2), dev_x), (pl.ds(rows // 2, rows // 2), dev_x2)


    @pl.when(c == 1)
    def _():
        def fx(f):
            with stage("fyfin"):
                fy[f].finish(XY.at[f])
                for h, to in halves(YF * T):
                    send(XY.at[f, 1 - xl, h, :], XYr.at[f, h, :], k_fx[f], to)

        for i in range(8 + 3 * LAG):
            if i < 8:
                f, t = i // 4, i % 4
                with stage(f"factor{i}"):
                    if i == 4:
                        loaded(2)
                    both(factor, i)
                    fz.start(i)
                    leave(fy[f], t)
            for s in (3, 2, 1):
                if 0 <= i - s * LAG < 8:
                    with stage(f"fz{s}"):
                        fz.step(s, i - s * LAG)
            if i == 4:
                with stage("fy0mid"):
                    fy[0].middle()
            if i == 8:
                with stage("fy1mid"):
                    fy[1].middle()
            if i in AT_FX:
                fx(AT_FX.index(i))
        with stage("fxfin"):
            for f in range(2):
                arrived(XYr.at[f], k_fx[f])
                pieces(UY, f, 0, add(XY[f, xl], XYr[f]), YF)
            fyz.start()
        for t in range(4):
            with stage("fzfin"):
                for f in range(2):
                    v = fz.finish(4 * f + t)
                    for x in range(2):
                        VZ[order[t], 2 * x + f] = v[x]
                leave(fzy, t)
        with stage("fyzmid"):
            fyz.middle()
        with stage("fzymid"):
            fzy.middle()
        with stage("fyzfin"):
            HY[...] = fyz.finish()
            send(HY, HYr, k_fh, dev_xh)
        with stage("fzyfin"):
            fzy.finish(XZ)
            theirs = XZ.at[pl.ds(2 * (1 - xl), 2)]
            send(theirs, XZr.at[0], k_xz, dev_x)
            send(theirs, XZr.at[1], k_xz, dev_x2)
            send(XZ.at[pl.ds(2 * xl, 2)], XZr.at[2], k_xz, dev_xh)
        with stage("fhfin"):
            arrived(HYr, k_fh)
            FY[:, z] = add(HY[...], HYr[...])
            fay[0].start()
            fay[1].start()
        with stage("fxm"):
            arrived(XZr, k_xz)
            near = XZr[0].astype(F32) + XZr[1].astype(F32)
            FZ[:, z] = ((XZ[pl.ds(2 * xl, 2)].astype(F32) + XZr[2].astype(F32)) + near).astype(BF16)
            faz[0].start()
            faz[1].start()
        with stage("fayrelay"):
            fay[0].relay()
            fay[1].relay()
        with stage("fazrelay"):
            faz[0].relay()
            faz[1].relay()
        with stage("fafin"):
            fay[0].finish()
            send(FY.at[0], FY.at[0], k_fpy, core)
            faz[0].finish()
            send(FZ.at[0], FZ.at[0], k_fpz, core)
            fay[1].finish()
            faz[1].finish()

    @pl.when(c == 0)
    def _():
        kept, groups[:] = list(groups), []
        with stage("waitB"):
            loaded(2)
        for t in range(4):
            with stage("grad"):
                both(gradient, t)
                d = order[t]
                for h, to in halves(XB * T):
                    send(WX.at[1 - xl, d, h, :], RX.at[d, h, :], k_gx[t], to)
                leave(gy, t)
        for t in range(4):
            with stage("gx"):
                d = order[t]
                arrived(RX.at[d], k_gx[t])
                VX[d, 0] = add(WX[xl, d], RX[d])
                leave(gxy, t)
            if t == 1:
                with stage("gymid"):
                    gy.middle()
            if t == 2:
                with stage("gxymid"):
                    gxy.middle()
        with stage("gyfin"):
            gy.finish(XG)
            for h, to in halves(HB * T):
                send(XG.at[1 - xl, h, :], XGr.at[h, :], k_xg, to)
        with stage("gxyfin"):
            gxy.finish(YX)
            pieces(UG, 0, HB, YX[0], XB)
        with stage("gxfin"):
            arrived(XGr, k_xg)
            pieces(UG, 0, 0, add(XG[xl], XGr[...]), HB)
            gz.start()
        with stage("gzmid"):
            gz.middle()
        with stage("gzfin"):
            HG[...] = gz.finish()[0]
            send(HG, HGr, k_gh, dev_xh)
        with stage("ghfin"):
            arrived(HGr, k_gh)
            GA[z] = add(HG[...], HGr[...])
            ga.start()
        with stage("waitF"):
            arrived(FY.at[0], k_fpy)
            arrived(FZ.at[0], k_fpz)
        groupsG.extend(groups)
        groups[:] = kept

    with stage("damp"):
        for k, (p, q) in enumerate(UPPER):
            if k < ZF:
                block = FZ[c, :, 16 * k : 16 * (k + 1), :]
            else:
                block = FY[c, :, 16 * (k - ZF) : 16 * (k - ZF + 1), :]
            block = block.reshape(T, T).astype(F32)
            Fm[p * T : (p + 1) * T, q * T : (q + 1) * T] = block
            if p != q:
                Fm[q * T : (q + 1) * T, p * T : (p + 1) * T] = block.T
        eye = (
            lax.broadcasted_iota(jnp.int32, (D, D), 0) == lax.broadcasted_iota(jnp.int32, (D, D), 1)
        ).astype(F32)
        f = Fm[...]
        trace = jnp.sum(jnp.sum(f * eye, axis=0, keepdims=True), axis=1, keepdims=True)
        damped = f + (trace * (0.05 / D)) * eye
        square = jnp.sum(jnp.sum(damped * damped, axis=0, keepdims=True), axis=1, keepdims=True)
        inverse_size = 1.0 / jnp.sqrt(square + 1e-06)
        Pm[...] = eye - damped * inverse_size

    with stage("ns1"):
        r = split(Pm[...])
        Fm[...] = dot3(r, r)
    @pl.when(c == 0)
    def _():
        kept, groups[:] = list(groups), groupsG
        with stage("garelay"):
            ga.relay()
            arrived(GA.at[pl.ds(0, 2)], ga.k[0])
            for far in (0, 1, 2, 6, 7):
                remote(GA.at[(z + far) % NZ], GA.at[(z + far) % NZ], k_gp, core, LAST + 5).start()
        groupsG[:], groups[:] = list(groups), kept

    with stage("ns2"):
        r1 = split(Fm[...])
        Qm[...] = dot3(r1, r1)

    with stage("ns3"):
        Pm[...] = eye + Pm[...] + Fm[...] + dot3(r, r1)

    with stage("ns4"):
        r2 = split(Qm[...])
        Fm[...] = dot3(r2, r2)
        Pm[...] = Pm[...] + dot3(split(Pm[...]), r2)

    @pl.when(c == 0)
    def _():
        with stage("gafin"):
            arrived(GA.at[pl.ds(0, 3)], ga.k[2])
            for far in (3, 4, 5):
                remote(GA.at[(z + far) % NZ], GA.at[(z + far) % NZ], k_gp, core, LAST + 5).start()

    with stage("ns5"):
        r3 = split(Fm[...])
        X[0], X[1] = split((Pm[...] + dot3(split(Pm[...]), r3)) * inverse_size)

    lo, hi = pl.ds(0, R), pl.ds(R, R)
    out_lo, out_hi = out.at[0, lo, :], out.at[0, hi, :]

    def gather():
        for k in range(GB):
            p, q = k // 4, k % 4
            Gm[p * T : (p + 1) * T, q * T : (q + 1) * T] = GA[:, 16 * k : 16 * (k + 1), :].reshape(T, T)

    @pl.when(c == 1)
    def _():
        remote(X, Xp, k_x, core, LAST + 3).start()
        with stage("waitG"):
            arrived(GA, k_gp)
        with stage("gather"):
            gather()
            right = split(dot(Gm[...], X[0]) + dot(Gm[...], X[1]))
        with stage("waitX"):
            arrived(Xp.at[:, hi, :], k_x)
        with stage("last"):
            mine[...] = dot3((Xp[0, hi, :], Xp[1, hi, :]), right).astype(BF16)
            remote(mine, out_hi, k_out, core, LAST + 4).start()
            pltpu.make_async_copy(mine, out_hi, local_sem.at[3]).start()
        with stage("drain"):
            remote(X, Xp, k_x, core, LAST + 3).wait_send()
            sent(groups)

    @pl.when(c == 0)
    def _():
        theirs = X.at[:, hi, :], Xp.at[:, hi, :]
        remote(*theirs, k_x, core, LAST + 3).start()
        with stage("gather"):
            gather()
            left = split(dot(X[0, lo, :], Gm[...]) + dot(X[1, lo, :], Gm[...]))
        with stage("waitX"):
            arrived(Xp, k_x)
        with stage("last"):
            mine[...] = dot3(left, (Xp[0], Xp[1])).astype(BF16)
            remote(mine, out_lo, k_out, core, LAST + 4).start()
            pltpu.make_async_copy(mine, out_lo, local_sem.at[3]).start()
        with stage("drain"):
            remote(*theirs, k_x, core, LAST + 3).wait_send()
            remote(GA, GA, k_gp, core, LAST + 5).wait_send()
            sent(groupsG)

    with stage("waitO"):
        pltpu.make_async_copy(mine, out_lo, local_sem.at[3]).wait()
        arrived(out_lo, k_out)
        remote(mine, out_lo, k_out, core, LAST + 4).wait_send()
        for src, dst, k, g in gets:
            remote(src, dst, k, core, g).wait_send()
    assert used[0] == NSEM, used[0]


FENCE = True
LAG = 3
AT_FX = (9, 12)
SENT = 2 * 1024 * 1024
NSEM = 79
LAST = 6
NSEND = LAST + 6


def local_step(edge_in, edge_grad, row_mask, layer_at):
    def v(*shape, dtype=BF16):
        return pltpu.VMEM(shape, dtype)

    def ystage(m, rows):
        return [v(4, m, rows, T), v(2, m, rows // 2, T), v(2, 2, m, rows // 2, T)]

    def zpair(m, rows):
        return [v(NZ, 1, m, rows, T), v(3, m, rows, T), v(4, m, rows, T)]

    def zring(chunks, m, rows):
        return [v(NZ, chunks, m, rows, T), v(4, chunks, 2, m, rows, T)]

    yf, hb, xb = YF * T, HB * T, XB * T
    any_ = pl.BlockSpec(memory_space=pl.ANY)
    return pl.pallas_call(
        kernel,
        out_shape=pltpu.VMEM((1, D, D), BF16),
        in_specs=[pl.BlockSpec(memory_space=pltpu.SMEM), any_, any_, any_],
        out_specs=any_,
        scratch_shapes=[
            v(L, 2 * R, dtype=jnp.int32), v(L, 2 * R, D), v(L, 2 * R, D), v(SENT // (2 * D), D),
            *zring(8, 2, ZP), *ystage(4, ZP), v(4, ZP, T), v(3, 2, ZP, T),
            *ystage(2, yf), *ystage(2, yf), v(2, 2, yf, T), v(2, yf, T), *zpair(2, YP), v(2, YP, T), v(2, YP, T),
            v(2, NZ, ZP, T), v(2, NZ, YP, T),
            *ystage(2, hb), v(2, hb, T), v(hb, T), v(2, 4, xb, T), v(4, xb, T), *ystage(1, xb), v(1, xb, T),
            *zpair(1, GP), v(GP, T), v(GP, T), v(NZ, GP, T),
            v(D, D, dtype=F32), v(D, D, dtype=F32), v(D, D, dtype=F32), v(D, D), v(2, D, D), v(2, D, D), v(R, D),
            pltpu.SemaphoreType.DMA((4,)), pltpu.SemaphoreType.DMA((NSEND,)), pltpu.SemaphoreType.DMA((NSEM,)),
        ],
        compiler_params=pltpu.CompilerParams(
            collective_id=0, has_side_effects=True, vmem_limit_bytes=60 * 1024 * 1024
        ),
    )(layer_at, row_mask, edge_in, edge_grad)


def solution(mesh):
    rows = P(None, ("dp", "owner"), None)
    return jax.shard_map(
        local_step, mesh=mesh, in_specs=(rows, rows, P(None, ("dp", "owner")), P()),
        out_specs=P("owner", None, None), check_vma=False,
    )
```

```python
import contextlib
import math

import jax
import jax.numpy as jnp
from jax import lax
from jax.experimental import pallas as pl
from jax.experimental.pallas import tpu as pltpu
from jax.sharding import PartitionSpec as P

MESH = pl.DeviceIdType.MESH
F32 = jnp.float32
BF16 = jnp.bfloat16
L = 8
D = 512
R = 256
NZ = 8
T = 128
UPPER = [(i, j) for i in range(4) for j in range(i, 4)]
NF = len(UPPER)
ZF = 7
YF = NF - ZF
ZP, YP = 16 * ZF, 16 * YF
GB = 16
HB = 4
XB = GB - HB
GP = 16 * GB


def add(a, b):
    return (a.astype(F32) + b.astype(F32)).astype(BF16)


def split(x):
    hi = x.astype(BF16)
    return hi, (x - hi.astype(F32)).astype(BF16)


def dot(a, b):
    return lax.dot_general(a, b, (((1,), (0,)), ((), ())), preferred_element_type=F32)


def stack(a, b):
    return tuple(jnp.concatenate(p, axis=0) for p in zip(a, b))


def dot3(a, b):
    (ah, al), (bh, bl) = a, b
    return dot(ah, bh) + (dot(ah, bl) + dot(al, bh))


def kernel(
    layer_at, mask_hbm, in_hbm, grad_hbm, out,
    mask, rows_in, rows_grad, dummy,
    WZ, RZ, VZ, RZr, RZd, XZ, XZr,
    WY0, RY0r, RY0d, WY1, RY1r, RY1d, XY, XYr, UY, RUr, RUd, HY, HYr, FZ, FY,
    WG, RGr, RGd, XG, XGr, WX, RX, VX, RXr, RXd, YX, UG, RUGr, RUGd, HG, HGr, GA,
    Fm, Pm, Qm, Gm, X, Xp, mine, local_sem, send_sem, recv_sem,
):
    dp, ow = lax.axis_index("dp"), lax.axis_index("owner")
    z, xh, c = dp // 4, (dp // 2) % 2, dp % 2
    xl, y = ow // 4, ow % 4

    def dev(z=z, xh=xh, c=c, xl=xl, y=y):
        return (z * 4 + xh * 2 + c, xl * 4 + y)

    ya = y + 1 - 2 * (y % 2)
    yb = 3 - y
    yo = (y + 2) % 4
    core = dev(c=1 - c)
    dev_ya, dev_yb = dev(y=ya), dev(y=yb)
    dev_x, dev_x2, dev_xh = dev(xl=1 - xl), dev(xl=1 - xl, xh=1 - xh), dev(xh=1 - xh)
    up, down = dev(z=(z + 1) % NZ), dev(z=(z + NZ - 1) % NZ)

    used = [0]
    groups, groupsG = [], []

    def ids():
        used[0] += 1
        return used[0] - 1

    def remote(src, dst, k, to, g=0):
        return pltpu.make_async_remote_copy(
            src_ref=src, dst_ref=dst, send_sem=send_sem.at[g], recv_sem=recv_sem.at[k],
            device_id=to, device_id_type=MESH,
        )

    def send(src, dst, k, to):
        size = math.prod(src.shape) * src.dtype.itemsize
        if not groups or groups[-1] + size > SENT:
            groups.append(0)
        groups[-1] += size
        remote(src, dst, k, to, len(groups) - 1).start()

    def sent(groups):
        for g, size in enumerate(groups):
            ref = dummy.at[pl.ds(0, size // (2 * D))]
            pltpu.make_async_copy(ref, ref, send_sem.at[g]).wait()
        assert len(groups) <= LAST, len(groups)

    def arrived(dst, k):
        remote(dst, dst, k, core).wait_recv()

    @contextlib.contextmanager
    def stage(name):
        with jax.named_scope(name):
            yield
        if FENCE:
            pl.delay(1)

    barrier = pltpu.get_barrier_semaphore()
    up2, down2 = dev(z=(z + 2) % NZ), dev(z=(z + NZ - 2) % NZ)
    peers = (core, dev_ya, dev_yb, dev_x, dev_x2, dev_xh, up, down, up2, down2)
    for peer in peers:
        pl.semaphore_signal(barrier, inc=1, device_id=peer, device_id_type=MESH)

    own, other = pl.ds(0, R), pl.ds(R, R)
    loads = ((mask_hbm, mask.at[:, own]), (in_hbm, rows_in.at[:, own, :]), (grad_hbm, rows_grad.at[:, own, :]))
    gets = [(mask_hbm, mask.at[:, other]), (in_hbm, rows_in.at[:, other, :]), (grad_hbm, rows_grad.at[:, other, :])]
    gets = [(src, dst, ids(), LAST + i) for i, (src, dst) in enumerate(gets)]
    for i, (src, dst) in enumerate(loads):
        pltpu.make_async_copy(src, dst, local_sem.at[i]).start()
    with stage("barrier"):
        pl.semaphore_wait(barrier, len(peers))
        for src, dst, k, g in gets:
            remote(src, dst, k, core, g).start()

    def loaded(i):
        src, dst = loads[i]
        pltpu.make_async_copy(src, dst, local_sem.at[i]).wait()
        arrived(gets[i][1], gets[i][2])

    with stage("waitA"):
        loaded(0)
        loaded(1)

    dirs = ((1, up, up2), (-1, down, down2))

    def zd(direction, far):
        return (z + NZ + direction * far) % NZ

    class ZRing:
        def __init__(self, W, Rz, rows, chunks):
            self.W, self.Rz = W, Rz
            self.k = [[ids() for _ in range(chunks)] for _ in range(4)]
            self.half = [pl.ds(0, rows // 2), pl.ds(rows // 2, rows // 2)]

        def go(self, n, s, q, half=None):
            w, r = self.W.at[zd(dirs[n][0], 4 - s), q], self.Rz.at[s, q, n]
            if half is not None:
                w, r = w.at[:, half, :], r.at[:, half, :]
            send(w, r, self.k[s][q], dirs[n][1])

        def start(self, q=0):
            for n in range(2):
                self.go(n, 0, q, self.half[n])
            for n in range(2):
                self.go(n, 1, q, self.half[1 - n])

        def step(self, s, q=0):
            arrived(self.Rz.at[s - 1, q, 0] if s == 1 else self.Rz.at[s - 1, q], self.k[s - 1][q])
            for n in range(2):
                d = zd(dirs[n][0], 4 - s)
                if s == 1:
                    h = self.half[n]
                    self.W[d, q, :, h, :] = add(self.W[d, q, :, h, :], self.Rz[0, q, n, :, h, :])
                    self.go(n, 1, q, h)
                else:
                    self.W[d, q] = add(self.W[d, q], self.Rz[s - 1, q, n])
                    self.go(n, s, q)

        def finish(self, q=0):
            arrived(self.Rz.at[3, q], self.k[3][q])
            mine = self.W[z, q].astype(F32)
            return (mine + (self.Rz[3, q, 0].astype(F32) + self.Rz[3, q, 1].astype(F32))).astype(BF16)

    class YStage:
        def __init__(self, W, Rr, Rd, rows):
            self.W, self.Rr, self.Rd = W, Rr, Rd
            self.kr, self.kd = ids(), ids()
            h = rows // 2
            self.half = [pl.ds(0, h), pl.ds(h, h)]

        def relay(self):
            for s, to in enumerate((dev_ya, dev_yb)):
                send(self.W.at[yo, :, self.half[s], :], self.Rr.at[s], self.kr, to)

        def direct(self, s):
            d, to = ((ya, dev_ya), (yb, dev_yb))[s]
            send(self.W.at[d, :, self.half[s], :], self.Rd.at[0, s], self.kd, to)

        def start(self):
            self.relay()
            self.direct(0)
            self.direct(1)

        def middle(self):
            arrived(self.Rr, self.kr)
            for s, (d, to) in enumerate(((yb, dev_yb), (ya, dev_ya))):
                h = self.half[s]
                self.W[d, :, h, :] = add(self.W[d, :, h, :], self.Rr[s])
                send(self.W.at[d, :, h, :], self.Rd.at[1, s], self.kd, to)

        def finish(self, out):
            arrived(self.Rd, self.kd)
            for s in range(2):
                h = self.half[s]
                total = self.W[y, :, h, :].astype(F32) + (self.Rd[0, s].astype(F32) + self.Rd[1, s].astype(F32))
                out[:, h, :] = total.astype(BF16)

    class ZPair:
        def __init__(self, W, Rr, Rd, rows):
            self.W, self.Rr, self.Rd, self.kr, self.kd = W, Rr, Rd, ids(), ids()
            self.half = [pl.ds(0, rows // 2), pl.ds(rows // 2, rows // 2)]

        def start(self):
            W, Rr = self.W, self.Rr
            for n, (direction, to, to2) in enumerate(dirs):
                h = self.half[n]
                send(W.at[zd(direction, 4), 0, :, h, :], Rr.at[2, :, h, :], self.kr, to2)
                send(W.at[zd(direction, 3), 0], Rr.at[n], self.kr, to)
            for n, (direction, to, to2) in enumerate(dirs):
                send(W.at[zd(direction, 1), 0], self.Rd.at[n], self.kd, to)

        def middle(self):
            W, Rr = self.W, self.Rr
            arrived(Rr, self.kr)
            for n, (direction, to, to2) in enumerate(dirs):
                d = zd(direction, 2)
                near, far = self.half[1 - n], self.half[n]
                W[d, 0, :, near, :] = add(W[d, 0, :, near, :], Rr[n, :, near, :])
                both = Rr[n, :, far, :].astype(F32) + Rr[2, :, far, :].astype(F32)
                W[d, 0, :, far, :] = (W[d, 0, :, far, :].astype(F32) + both).astype(BF16)
                send(W.at[d, 0], self.Rd.at[2 + n], self.kd, to2)

        def finish(self):
            Rd = self.Rd
            arrived(Rd, self.kd)
            near = Rd[0].astype(F32) + Rd[1].astype(F32)
            far = Rd[2].astype(F32) + Rd[3].astype(F32)
            return ((self.W[z, 0].astype(F32) + near) + far).astype(BF16)

    class AllGather:
        def __init__(self, A, rows):
            self.A, self.k = A, [ids() for _ in range(3)]
            self.half = [pl.ds(0, rows // 2), pl.ds(rows // 2, rows // 2)]

        def start(self):
            p = self.A.at[z]
            for direction, to, to2 in dirs:
                send(p, p, self.k[1], to2)
            for direction, to, to2 in dirs:
                send(p, p, self.k[0], to)

        def relay(self):
            arrived(self.A.at[pl.ds(0, 2)], self.k[1])
            for n, (direction, to, to2) in enumerate(dirs):
                p = self.A.at[zd(-direction, 2), self.half[n], :]
                send(p, p, self.k[2], to2)
            for n, (direction, to, to2) in enumerate(dirs):
                p = self.A.at[zd(-direction, 2)]
                send(p, p, self.k[2], to)

        def finish(self):
            arrived(self.A.at[pl.ds(0, 2)], self.k[0])
            arrived(self.A.at[pl.ds(0, 3)], self.k[2])

    order = (yo, ya, yb, y)
    fz = ZRing(WZ, RZ, ZP, 8)
    fzy = YStage(VZ, RZr, RZd, ZP)
    fy = (YStage(WY0, RY0r, RY0d, YF * T), YStage(WY1, RY1r, RY1d, YF * T))
    fyz = ZPair(UY, RUr, RUd, YP)
    faz = (AllGather(FZ.at[0], ZP), AllGather(FZ.at[1], ZP))
    fay = (AllGather(FY.at[0], YP), AllGather(FY.at[1], YP))
    gy = YStage(WG, RGr, RGd, HB * T)
    gxy = YStage(VX, RXr, RXd, XB * T)
    gz = ZPair(UG, RUGr, RUGd, GP)
    ga = AllGather(GA, GP)
    k_fx = [ids() for _ in range(2)]
    k_gx = [ids() for _ in range(4)]
    k_xz, k_fh, k_gh, k_xg = (ids() for _ in range(4))
    k_fpz, k_fpy, k_gp, k_x, k_out = (ids() for _ in range(5))

    def pieces(ref, m, first, f, n):
        for k in range(n):
            ref[:, 0, m, 16 * (first + k) : 16 * (first + k + 1), :] = f[k * T : (k + 1) * T].reshape(8, 16, T)

    def factor(i, x):
        f, t = i // 4, i % 4
        d = order[t]
        layer = layer_at[x * 4 + d]
        a = (rows_in, rows_grad)[f][layer]
        m = mask[pl.ds(layer, 1), :].astype(F32).astype(BF16)
        am = a.T * m
        top = dot(am[:R], a) * (1.0 / 65536)
        low = dot(am[R:], a[:, R:]) * (1.0 / 65536)
        for k, (p, q) in enumerate(UPPER):
            if p < 2:
                block = top[p * T : (p + 1) * T, q * T : (q + 1) * T].astype(BF16)
            else:
                block = low[(p - 2) * T : (p - 1) * T, (q - 2) * T : (q - 1) * T].astype(BF16)
            if k < ZF:
                WZ[:, i, x, 16 * k : 16 * (k + 1), :] = block.reshape(8, 16, T)
            else:
                (WY0, WY1)[f][d, x, (k - ZF) * T : (k - ZF + 1) * T, :] = block

    def gradient(t, x):
        d = order[t]
        layer = layer_at[x * 4 + d]
        g = (dot(rows_in[layer].T, rows_grad[layer]) * (1.0 / 256)).astype(BF16)
        for k in range(GB):
            p, q = k // 4, k % 4
            block = g[p * T : (p + 1) * T, q * T : (q + 1) * T]
            if k < HB:
                WG[d, x, k * T : (k + 1) * T, :] = block
            else:
                WX[x, d, (k - HB) * T : (k - HB + 1) * T, :] = block

    def both(f, t):
        lax.fori_loop(0, 2, lambda x, carry: (f(t, x), carry)[1], 0)

    def leave(ystage, t):
        if t == 0:
            ystage.relay()
        elif t < 3:
            ystage.direct(t - 1)

    def halves(rows):
        return (pl.ds(0, rows // 2), dev_x), (pl.ds(rows // 2, rows // 2), dev_x2)


    @pl.when(c == 1)
    def _():
        def fx(f):
            with stage("fyfin"):
                fy[f].finish(XY.at[f])
                for h, to in halves(YF * T):
                    send(XY.at[f, 1 - xl, h, :], XYr.at[f, h, :], k_fx[f], to)

        for i in range(8 + 3 * LAG):
            if i < 8:
                f, t = i // 4, i % 4
                with stage(f"factor{i}"):
                    if i == 4:
                        loaded(2)
                    both(factor, i)
                    fz.start(i)
                    leave(fy[f], t)
            for s in (3, 2, 1):
                if 0 <= i - s * LAG < 8:
                    with stage(f"fz{s}"):
                        fz.step(s, i - s * LAG)
            if i == 4:
                with stage("fy0mid"):
                    fy[0].middle()
            if i == 8:
                with stage("fy1mid"):
                    fy[1].middle()
            if i in AT_FX:
                fx(AT_FX.index(i))
        with stage("fxfin"):
            for f in range(2):
                arrived(XYr.at[f], k_fx[f])
                pieces(UY, f, 0, add(XY[f, xl], XYr[f]), YF)
            fyz.start()
        for t in range(4):
            with stage("fzfin"):
                for f in range(2):
                    v = fz.finish(4 * f + t)
                    for x in range(2):
                        VZ[order[t], 2 * x + f] = v[x]
                leave(fzy, t)
        with stage("fyzmid"):
            fyz.middle()
        with stage("fzymid"):
            fzy.middle()
        with stage("fyzfin"):
            HY[...] = fyz.finish()
            send(HY, HYr, k_fh, dev_xh)
        with stage("fzyfin"):
            fzy.finish(XZ)
            theirs = XZ.at[pl.ds(2 * (1 - xl), 2)]
            send(theirs, XZr.at[0], k_xz, dev_x)
            send(theirs, XZr.at[1], k_xz, dev_x2)
            send(XZ.at[pl.ds(2 * xl, 2)], XZr.at[2], k_xz, dev_xh)
        with stage("fhfin"):
            arrived(HYr, k_fh)
            FY[:, z] = add(HY[...], HYr[...])
            fay[0].start()
            fay[1].start()
        with stage("fxm"):
            arrived(XZr, k_xz)
            near = XZr[0].astype(F32) + XZr[1].astype(F32)
            FZ[:, z] = ((XZ[pl.ds(2 * xl, 2)].astype(F32) + XZr[2].astype(F32)) + near).astype(BF16)
            faz[0].start()
            faz[1].start()
        with stage("fayrelay"):
            fay[0].relay()
            fay[1].relay()
        with stage("fazrelay"):
            faz[0].relay()
            faz[1].relay()
        with stage("fafin"):
            fay[0].finish()
            send(FY.at[0], FY.at[0], k_fpy, core)
            faz[0].finish()
            send(FZ.at[0], FZ.at[0], k_fpz, core)
            fay[1].finish()
            faz[1].finish()

    @pl.when(c == 0)
    def _():
        kept, groups[:] = list(groups), []
        with stage("waitB"):
            loaded(2)
        for t in range(4):
            with stage("grad"):
                both(gradient, t)
                d = order[t]
                for h, to in halves(XB * T):
                    send(WX.at[1 - xl, d, h, :], RX.at[d, h, :], k_gx[t], to)
                leave(gy, t)
        for t in range(4):
            with stage("gx"):
                d = order[t]
                arrived(RX.at[d], k_gx[t])
                VX[d, 0] = add(WX[xl, d], RX[d])
                leave(gxy, t)
            if t == 1:
                with stage("gymid"):
                    gy.middle()
            if t == 2:
                with stage("gxymid"):
                    gxy.middle()
        with stage("gyfin"):
            gy.finish(XG)
            for h, to in halves(HB * T):
                send(XG.at[1 - xl, h, :], XGr.at[h, :], k_xg, to)
        with stage("gxyfin"):
            gxy.finish(YX)
            pieces(UG, 0, HB, YX[0], XB)
        with stage("gxfin"):
            arrived(XGr, k_xg)
            pieces(UG, 0, 0, add(XG[xl], XGr[...]), HB)
            gz.start()
        with stage("gzmid"):
            gz.middle()
        with stage("gzfin"):
            HG[...] = gz.finish()[0]
            send(HG, HGr, k_gh, dev_xh)
        with stage("ghfin"):
            arrived(HGr, k_gh)
            GA[z] = add(HG[...], HGr[...])
            ga.start()
        with stage("waitF"):
            arrived(FY.at[0], k_fpy)
            arrived(FZ.at[0], k_fpz)
        groupsG.extend(groups)
        groups[:] = kept

    with stage("damp"):
        for k, (p, q) in enumerate(UPPER):
            if k < ZF:
                block = FZ[c, :, 16 * k : 16 * (k + 1), :]
            else:
                block = FY[c, :, 16 * (k - ZF) : 16 * (k - ZF + 1), :]
            block = block.reshape(T, T).astype(F32)
            Fm[p * T : (p + 1) * T, q * T : (q + 1) * T] = block
            if p != q:
                Fm[q * T : (q + 1) * T, p * T : (p + 1) * T] = block.T
        eye = (
            lax.broadcasted_iota(jnp.int32, (D, D), 0) == lax.broadcasted_iota(jnp.int32, (D, D), 1)
        ).astype(F32)
        f = Fm[...]
        trace = jnp.sum(jnp.sum(f * eye, axis=0, keepdims=True), axis=1, keepdims=True)
        damped = f + (trace * (0.05 / D)) * eye
        square = jnp.sum(jnp.sum(damped * damped, axis=0, keepdims=True), axis=1, keepdims=True)
        inverse_size = 1.0 / jnp.sqrt(square + 1e-06)
        Pm[...] = eye - damped * inverse_size

    with stage("ns1"):
        r = split(Pm[...])
        Fm[...] = dot3(r, r)
    @pl.when(c == 0)
    def _():
        kept, groups[:] = list(groups), groupsG
        with stage("garelay"):
            ga.relay()
            arrived(GA.at[pl.ds(0, 2)], ga.k[0])
            for far in (0, 1, 2, 6, 7):
                remote(GA.at[(z + far) % NZ], GA.at[(z + far) % NZ], k_gp, core, LAST + 5).start()
        groupsG[:], groups[:] = list(groups), kept

    with stage("ns2"):
        r1 = split(Fm[...])
        two = dot3(stack(r1, r), r1)
        Qm[...] = two[:D]
        Pm[...] = eye + Pm[...] + Fm[...] + two[D:]

    with stage("ns4"):
        r2 = split(Qm[...])
        two = dot3(stack(r2, split(Pm[...])), r2)
        Fm[...] = two[:D]
        Pm[...] = Pm[...] + two[D:]

    @pl.when(c == 0)
    def _():
        with stage("gafin"):
            arrived(GA.at[pl.ds(0, 3)], ga.k[2])
            for far in (3, 4, 5):
                remote(GA.at[(z + far) % NZ], GA.at[(z + far) % NZ], k_gp, core, LAST + 5).start()

    with stage("ns5"):
        r3 = split(Fm[...])
        X[0], X[1] = split((Pm[...] + dot3(split(Pm[...]), r3)) * inverse_size)

    lo, hi = pl.ds(0, R), pl.ds(R, R)
    out_lo, out_hi = out.at[0, lo, :], out.at[0, hi, :]

    def gather():
        for k in range(GB):
            p, q = k // 4, k % 4
            Gm[p * T : (p + 1) * T, q * T : (q + 1) * T] = GA[:, 16 * k : 16 * (k + 1), :].reshape(T, T)

    @pl.when(c == 1)
    def _():
        remote(X, Xp, k_x, core, LAST + 3).start()
        with stage("waitG"):
            arrived(GA, k_gp)
        with stage("gather"):
            gather()
            right = split(dot(Gm[...], X[0]) + dot(Gm[...], X[1]))
        with stage("waitX"):
            arrived(Xp.at[:, hi, :], k_x)
        with stage("last"):
            mine[...] = dot3((Xp[0, hi, :], Xp[1, hi, :]), right).astype(BF16)
            remote(mine, out_hi, k_out, core, LAST + 4).start()
            pltpu.make_async_copy(mine, out_hi, local_sem.at[3]).start()
        with stage("drain"):
            remote(X, Xp, k_x, core, LAST + 3).wait_send()
            sent(groups)

    @pl.when(c == 0)
    def _():
        theirs = X.at[:, hi, :], Xp.at[:, hi, :]
        remote(*theirs, k_x, core, LAST + 3).start()
        with stage("gather"):
            gather()
            left = split(dot(X[0, lo, :], Gm[...]) + dot(X[1, lo, :], Gm[...]))
        with stage("waitX"):
            arrived(Xp, k_x)
        with stage("last"):
            mine[...] = dot3(left, (Xp[0], Xp[1])).astype(BF16)
            remote(mine, out_lo, k_out, core, LAST + 4).start()
            pltpu.make_async_copy(mine, out_lo, local_sem.at[3]).start()
        with stage("drain"):
            remote(*theirs, k_x, core, LAST + 3).wait_send()
            remote(GA, GA, k_gp, core, LAST + 5).wait_send()
            sent(groupsG)

    with stage("waitO"):
        pltpu.make_async_copy(mine, out_lo, local_sem.at[3]).wait()
        arrived(out_lo, k_out)
        remote(mine, out_lo, k_out, core, LAST + 4).wait_send()
        for src, dst, k, g in gets:
            remote(src, dst, k, core, g).wait_send()
    assert used[0] == NSEM, used[0]


FENCE = True
LAG = 3
AT_FX = (9, 12)
SENT = 2 * 1024 * 1024
NSEM = 79
LAST = 6
NSEND = LAST + 6


def local_step(edge_in, edge_grad, row_mask, layer_at):
    def v(*shape, dtype=BF16):
        return pltpu.VMEM(shape, dtype)

    def ystage(m, rows):
        return [v(4, m, rows, T), v(2, m, rows // 2, T), v(2, 2, m, rows // 2, T)]

    def zpair(m, rows):
        return [v(NZ, 1, m, rows, T), v(3, m, rows, T), v(4, m, rows, T)]

    def zring(chunks, m, rows):
        return [v(NZ, chunks, m, rows, T), v(4, chunks, 2, m, rows, T)]

    yf, hb, xb = YF * T, HB * T, XB * T
    any_ = pl.BlockSpec(memory_space=pl.ANY)
    return pl.pallas_call(
        kernel,
        out_shape=pltpu.VMEM((1, D, D), BF16),
        in_specs=[pl.BlockSpec(memory_space=pltpu.SMEM), any_, any_, any_],
        out_specs=any_,
        scratch_shapes=[
            v(L, 2 * R, dtype=jnp.int32), v(L, 2 * R, D), v(L, 2 * R, D), v(SENT // (2 * D), D),
            *zring(8, 2, ZP), *ystage(4, ZP), v(4, ZP, T), v(3, 2, ZP, T),
            *ystage(2, yf), *ystage(2, yf), v(2, 2, yf, T), v(2, yf, T), *zpair(2, YP), v(2, YP, T), v(2, YP, T),
            v(2, NZ, ZP, T), v(2, NZ, YP, T),
            *ystage(2, hb), v(2, hb, T), v(hb, T), v(2, 4, xb, T), v(4, xb, T), *ystage(1, xb), v(1, xb, T),
            *zpair(1, GP), v(GP, T), v(GP, T), v(NZ, GP, T),
            v(D, D, dtype=F32), v(D, D, dtype=F32), v(D, D, dtype=F32), v(D, D), v(2, D, D), v(2, D, D), v(R, D),
            pltpu.SemaphoreType.DMA((4,)), pltpu.SemaphoreType.DMA((NSEND,)), pltpu.SemaphoreType.DMA((NSEM,)),
        ],
        compiler_params=pltpu.CompilerParams(
            collective_id=0, has_side_effects=True, vmem_limit_bytes=60 * 1024 * 1024
        ),
    )(layer_at, row_mask, edge_in, edge_grad)


def solution(mesh):
    rows = P(None, ("dp", "owner"), None)
    return jax.shard_map(
        local_step, mesh=mesh, in_specs=(rows, rows, P(None, ("dp", "owner")), P()),
        out_specs=P("owner", None, None), check_vma=False,
    )
```
